256 devices in a mesh: seq: 8 (over y, x_lo), exp: 32 (over z, x_hi, core).
Axes of the slice: x: 4 (x_hi: 2, x_lo: 2; x = x_hi * 2 + x_lo), y: 4, z: 8, core: 2. Of those that a mesh axis runs over, the one named last changes fastest.
Arguments:
- tokens: bfloat16 [65536, 2048], P(('seq', 'exp')), may hold values from -128 to 128
- slot_embed: bfloat16 [2048, 256], P(None, 'exp'), may hold values from -0.397747564 to 0.397747564
- expert_in: bfloat16 [64, 2048, 4096], P('exp', None, 'seq'), may hold values from -0.125 to 0.125
- expert_out: bfloat16 [64, 4096, 2048], P('exp', 'seq'), may hold values from -0.09375 to 0.09375
- out_grad: bfloat16 [65536, 2048], P(('seq', 'exp')), may hold values from -0.59765625 to 0.59765625
Outputs:
- tok_grad: bfloat16 [65536, 2048], P(('seq', 'exp'))
- slot_grad: float32 [2048, 256], P('seq', 'exp')
The draws below stay inside these ranges and needn't reach their ends.
All inputs are finite; a program needn't handle non-finite values.
Results may differ from the reference program's by a relative error of at most 0.024.
Values may be sent and summed in bfloat16 or wider, within the bound.
A program may use at most 64 MiB of HBM per device.

```python
import math
from functools import partial
import jax
import jax.numpy as jnp
from jax import lax

D = 2048
H = 4096
SLOTS = 4
EXPERTS = 64
S = 256
TOKENS = 65536


def slot_values(key):
    normal_draw = jax.random.normal(jax.random.fold_in(key, 101), (D, S), jnp.float32)
    return jnp.clip(normal_draw, -6.0, 6.0) * (3.0 / math.sqrt(D))


def draw_slot_embed(key, part):
    return slot_values(key).astype(jnp.bfloat16)


def draw_tokens(key, part):
    values = jnp.clip(jax.random.normal(jax.random.fold_in(key, 202), (TOKENS, D), jnp.float32), -6.0, 6.0)
    return jnp.clip(values, -128.0, 128.0).astype(jnp.bfloat16)


def block_levels(key, extent, shards, least, high):
    loudness, own = 1.0, jax.random.fold_in(key, 6)
    for position, shards_of in shards:
        steps = jnp.exp(jax.random.uniform(jax.random.fold_in(own, position), (shards_of,), jnp.float32, least / len(shards), high / len(shards)))
        loudness = loudness * jnp.repeat(steps, extent[position] // shards_of).reshape([-1 if axis == position else 1 for axis in range(len(extent))])
    return loudness


def centred(key, dims, spread, bound, cuts=(), kind=jnp.bfloat16):
    entries = spread * jax.random.normal(key, dims, jnp.float32)
    if cuts:
        entries = entries * block_levels(key, dims, cuts, -0.22, 0.18)
    return jnp.clip(entries, -bound, bound).astype(kind)


def setup_inputs(seed: int = 0) -> dict:
    seeds = jax.random.split(jax.random.key(seed), 6)
    tokens = draw_tokens(jax.random.fold_in(seeds[5], 71), 0)
    slot_embed = draw_slot_embed(jax.random.fold_in(seeds[5], 71), 0)
    expert_in = centred(seeds[2], (EXPERTS, D, H), D ** -0.5, 0.125, ((0, 32), (2, 8)))
    expert_out = centred(seeds[3], (EXPERTS, H, D), H ** -0.5, 0.09375, ((0, 32), (1, 8)))
    out_grad = centred(seeds[4], (TOKENS, D), 0.1, 0.59765625, ((0, 256),))
    return dict(tokens=tokens, slot_embed=slot_embed, expert_in=expert_in, expert_out=expert_out, out_grad=out_grad)


def contract_rows(left, right):
    return lax.dot_general(left, right, (((0,), (0,)), ((), ())), preferred_element_type=jnp.float32)

def contract_cols(left, right):
    return lax.dot_general(left, right, (((1,), (1,)), ((), ())), preferred_element_type=jnp.float32)

def expert_forward(operands):
    slot_rows, weight_in, weight_out = operands
    pre_act = jnp.dot(slot_rows, weight_in, preferred_element_type=jnp.float32)
    hidden = jax.nn.gelu(pre_act, approximate=True).astype(jnp.bfloat16)
    return (pre_act, jnp.dot(hidden, weight_out, preferred_element_type=jnp.float32))

def expert_backward(operands):
    grad_rows, pre_act, weight_in, weight_out = operands
    hid_grad = contract_cols(grad_rows, weight_out)
    _, pullback = jax.vjp(partial(jax.nn.gelu, approximate=True), pre_act)
    act_grad = pullback(hid_grad)[0].astype(jnp.bfloat16)
    return contract_cols(act_grad, weight_in)

def reference(tokens, slot_embed, expert_in, expert_out, out_grad):
    logits = jnp.dot(tokens, slot_embed, preferred_element_type=jnp.float32)
    col_top = lax.optimization_barrier(jnp.max(logits, axis=0))
    exponent = jnp.exp(logits - col_top)
    dispatch = exponent / lax.optimization_barrier(jnp.sum(exponent, axis=0))
    dispatch_b = dispatch.astype(jnp.bfloat16)
    combine_w = jax.nn.softmax(logits, axis=1)
    combine_b = combine_w.astype(jnp.bfloat16)
    slot_sum = contract_rows(dispatch_b, tokens)
    slot_in = slot_sum.astype(jnp.bfloat16).reshape(EXPERTS, SLOTS, D)
    pre_act, slot_part = lax.map(expert_forward, (slot_in, expert_in, expert_out))
    slot_out = slot_part.astype(jnp.bfloat16).reshape(S, D)
    comb_grad = contract_cols(out_grad, slot_out)
    grad_out = contract_rows(combine_b, out_grad).astype(jnp.bfloat16).reshape(EXPERTS, SLOTS, D)
    in_part = lax.map(expert_backward, (grad_out, pre_act, expert_in, expert_out))
    grad_in = in_part.astype(jnp.bfloat16).reshape(S, D)
    disp_grad = contract_cols(tokens, grad_in)
    centre = lax.optimization_barrier(jnp.sum(dispatch_b.astype(jnp.float32) * disp_grad, axis=0))
    comb_mean = lax.optimization_barrier(jnp.sum(combine_w * comb_grad, axis=1, keepdims=True))
    logit_grad = dispatch * (disp_grad - centre) + combine_w * (comb_grad - comb_mean)
    logit_b = logit_grad.astype(jnp.bfloat16)
    tok_grad = jnp.dot(dispatch_b, grad_in, preferred_element_type=jnp.float32) + contract_cols(logit_b, slot_embed)
    slot_grad = contract_rows(tokens, logit_b)
    return (tok_grad.astype(jnp.bfloat16), slot_grad)
```

```python
import functools

import jax
import jax.numpy as jnp
from jax import lax
from jax.experimental import pallas as pl
from jax.experimental.pallas import tpu as pltpu
from jax.sharding import Mesh
from jax.sharding import PartitionSpec as P

EXP = ("exp_0", "exp_1", "exp_2")
SEQ = ("seq_0", "seq_1")
SEQ_EXP = ("seq_0", "seq_1", "exp_0", "exp_1", "exp_2")
AXES = SEQ_EXP
F32, BF16 = jnp.float32, jnp.bfloat16
ROOT = 0.7978845608028654


def rows_dot(left, right):
    return lax.dot_general(left, right, (((1,), (0,)), ((), ())), preferred_element_type=F32)


def cols_dot(left, right):
    return lax.dot_general(left, right, (((1,), (1,)), ((), ())), preferred_element_type=F32)


def gelu_and_slope(v):
    t = jnp.tanh(ROOT * (v + 0.044715 * (v * v * v)))
    value = 0.5 * v * (1.0 + t)
    slope = 0.5 * (1.0 + t) + 0.5 * v * (1.0 - t * t) * (ROOT * (1.0 + 3.0 * 0.044715 * (v * v)))
    return value, slope


def flat(block):
    block = block.astype(F32)
    return block.reshape(-1, block.shape[-1])


def kernel(
    sizes,
    tok_hbm, slot_hbm, win_hbm, wout_hbm, og_hbm,
    tg_hbm, sg_out,
    tok, og, win, wout, tok_t, og_t, table, grads, logits, weight, comb_f, comb_g, disp_g,
    both, tg, factor,
    gath_a, gath_d,
    pb, pb1, pb2, pb3, rbc, rb1, rb2, rbz,
    pg, pg1, pg2, pg3, rgc, rg1, rg2, rgz,
    stat, stat_c, stat_1, stat_2, stat_z,
    cen, cen_z, cen_1, cen_2, cen_c,
    seq_in, seq_out, seq_rec,
    local_sem, send_sem, recv_sem,
):
    Y, XL, Z, XH, C = sizes
    N, NQ = XL * XH, Y * XL
    assert Y == N and C == 2
    S = C * XH * Z * 8
    W = tok.shape[1] // NQ
    HALF = W // 2
    ZR = Z * 8
    y, xl, z, xh, c = (lax.axis_index(name) for name in AXES)
    x, q = xh * XL + xl, y * XL + xl
    rem, div = lax.rem, lax.div

    def z_to(i):
        k = rem(z + i, Z)
        return k, {"exp_0": k}

    def y_to(i):
        k = rem(y + i, N)
        return k, {"seq_0": k}

    def x_to(i):
        k = rem(x + i, N)
        return k, {"exp_1": div(k, XL), "seq_1": rem(k, XL)}

    def q_to(i):
        k = rem(q + i, NQ)
        return k, {"seq_0": div(k, XL), "seq_1": rem(k, XL)}

    other = {"exp_2": 1 - c}
    MESH = pl.DeviceIdType.MESH
    count = [0]
    begun = []

    def send(src, dst, device):
        k = count[0]
        count[0] += 1
        copy = pltpu.make_async_remote_copy(
            src_ref=src, dst_ref=dst, send_sem=send_sem.at[k], recv_sem=recv_sem.at[k],
            device_id=device, device_id_type=MESH,
        )
        copy.start()
        begun.append(copy)
        return copy

    def arrive(copies):
        for copy in copies:
            copy.wait_recv()

    slot_copy = pltpu.make_async_copy
    first = [
        slot_copy(
            slot_hbm.at[:, pl.ds(pl.multiple_of(q * W + a * HALF, HALF), HALF)],
            gath_a.at[a, y, xl, c, xh, z],
            local_sem.at[a],
        )
        for a in range(2)
    ]
    big = [
        slot_copy(src, dst, local_sem.at[2 + k])
        for k, (src, dst) in enumerate(((tok_hbm, tok), (og_hbm, og), (win_hbm, win), (wout_hbm, wout)))
    ]
    for copy in first + big:
        copy.start()

    barrier = pltpu.get_barrier_semaphore()
    partners = [z_to(i)[1] for i in range(1, Z)]
    partners += [y_to(i)[1] for i in range(1, N)]
    partners += [x_to(i)[1] for i in range(1, N)]
    partners += [q_to(i)[1] for i in range(1, NQ)]
    partners += [other]
    for device in partners:
        pl.semaphore_signal(barrier, inc=1, device_id=device, device_id_type=MESH)
    pl.semaphore_wait(barrier, len(partners))

    def gather(buf, beside=None):
        moves = [send(buf.at[:, y, xl, c, xh, z], buf.at[:, y, xl, c, xh, z], z_to(i)[1]) for i in range(1, Z)]
        if beside:
            own, over_z, over_1, over_2, over_c = beside
            moves += [send(own.at[0], over_z.at[i - 1], z_to(i)[1]) for i in range(1, Z)]
        yield "sent"
        arrive(moves)
        moves = []
        for i in range(1, N):
            moves.append(send(buf.at[0, y, xl, c, xh], buf.at[0, y, xl, c, xh], x_to(i)[1]))
            moves.append(send(buf.at[1, y, xl, c, xh], buf.at[1, y, xl, c, xh], y_to(i)[1]))
        if beside:
            total = own[0]
            for i in range(1, Z):
                total += over_z[i - 1]
            own[1] = total
            moves += [send(own.at[1], over_1.at[i - 1], x_to(i)[1]) for i in range(1, N)]
        arrive(moves)
        moves = []
        for i in range(1, N):
            moves.append(send(buf.at[0, y, :, c], buf.at[0, y, :, c], y_to(i)[1]))
            moves.append(send(buf.at[1, :, xl, c, xh], buf.at[1, :, xl, c, xh], x_to(i)[1]))
        if beside:
            total = own[1]
            for i in range(1, N):
                total += over_1[i - 1]
            own[2] = total
            moves += [send(own.at[2], over_2.at[i - 1], y_to(i)[1]) for i in range(1, N)]
        arrive(moves)
        moves = [send(buf.at[:, :, :, c], buf.at[:, :, :, c], other)]
        if beside:
            total = own[2]
            for i in range(1, N):
                total += over_2[i - 1]
            own[3] = total
            moves += [send(own.at[3], over_c.at[0], other)]
        arrive(moves)

    lines = lax.broadcasted_iota(jnp.int32, (8, S), 0)

    def merge(entries):
        top = entries[0][0:1]
        for entry in entries[1:]:
            top = jnp.maximum(top, entry[0:1])
        scales = [jnp.exp(entry[0:1] - top) for entry in entries]
        total = entries[0][1:2] * scales[0]
        for entry, scale in zip(entries[1:], scales[1:]):
            total += entry[1:2] * scale
        turned = jnp.zeros((8, S), F32)
        for k, scale in enumerate(scales):
            turned = jnp.where(lines == k, scale, turned)
        factor[...] = jnp.concatenate([turned, jnp.zeros((120, S), F32)], axis=0).T
        return jnp.where(lines == 0, top, jnp.where(lines == 1, total, 0.0))

    def joined(parts, scaled, row, rows):
        total = None
        for k, part in enumerate(parts):
            part = flat(part)
            if scaled:
                part = part * factor[pl.ds(pl.multiple_of(row, 8), rows), k : k + 1]
            total = part if total is None else total + part
        return total

    def reduce(p, s1, s2, s3, rc, r1, r2, rz, scaled):
        w = p.shape[-1]
        moves = [send(p.at[:, 1 - c], rc, other)]
        if scaled:
            moves.append(send(stat.at[0], stat_c.at[0], other))
        yield "sent"
        arrive(moves)
        if scaled:
            stat[1] = merge([stat[0], stat_c[0]])

        def first_sum(b, _):
            for a in range(2):
                row = c * (S // 2) + div(rem(b, N), XL) * ZR
                total = joined((p[a, c, b], rc[a, b]), scaled and a == 0, row, ZR)
                s1[a, b] = total.reshape(Z, 8, w).astype(BF16)
            return 0

        lax.fori_loop(0, N * N, first_sum, 0)
        moves = []
        for i in range(1, N):
            k, device = y_to(i)
            moves.append(send(s1.at[0, pl.ds(k * N, N)], r1.at[0, i - 1], device))
            if scaled:
                moves.append(send(stat.at[1], stat_1.at[i - 1], device))
            k, device = x_to(i)
            moves.append(send(s1.at[1, pl.ds(k * N, N)], r1.at[1, i - 1], device))
        yield "sent"
        arrive(moves)
        if scaled:
            stat[2] = merge([stat[1]] + [stat_1[i] for i in range(N - 1)])

        def second_sum(b, _):
            for a, me in ((0, y), (1, x)):
                row = c * (S // 2) + div(b, XL) * ZR
                parts = [s1[a, me * N + b]] + [r1[a, i, b] for i in range(N - 1)]
                total = joined(parts, scaled and a == 0, row, ZR)
                s2[a, b] = total.reshape(Z, 8, w).astype(BF16)
            return 0

        lax.fori_loop(0, N, second_sum, 0)
        moves = []
        for i in range(1, N):
            k, device = x_to(i)
            moves.append(send(s2.at[0, k], r2.at[0, i - 1], device))
            if scaled:
                moves.append(send(stat.at[2], stat_2.at[i - 1], device))
            k, device = y_to(i)
            moves.append(send(s2.at[1, k], r2.at[1, i - 1], device))
        arrive(moves)
        if scaled:
            stat[3] = merge([stat[2]] + [stat_2[i] for i in range(N - 1)])
        for a, me in ((0, x), (1, y)):
            row = c * (S // 2) + xh * ZR
            parts = [s2[a, me]] + [r2[a, i] for i in range(N - 1)]
            total = joined(parts, scaled and a == 0, row, ZR)
            s3[a] = total.reshape(Z, 8, w).astype(BF16)
        moves = []
        for i in range(1, Z):
            k, device = z_to(i)
            moves.append(send(s3.at[:, k], rz.at[i - 1], device))
            if scaled:
                moves.append(send(stat.at[3], stat_z.at[i - 1], device))
        arrive(moves)
        if scaled:
            stat[4] = merge([stat[3]] + [stat_z[i] for i in range(Z - 1)])
        row = c * (S // 2) + xh * ZR + z * 8
        result = []
        for a in range(2):
            parts = [s3[a, z]] + [rz[i, a] for i in range(Z - 1)]
            result.append(joined(parts, scaled and a == 0, row, 8))
        yield result

    def end_of(steps):
        last = None
        for last in steps:
            pass
        return last

    own_row = pl.multiple_of(c * (S // 2) + xh * ZR + z * 8, 8)

    for copy in first:
        copy.wait()
    steps = gather(gath_a)
    next(steps)
    big[0].wait()
    tok_t[...] = tok[...].T
    big[1].wait()
    og_t[...] = og[...].T
    end_of(steps)

    def lay_table(k, _):
        for a in range(2):
            block = flat(gath_a[a, div(k, XL), rem(k, XL)]).astype(BF16)
            table[:, pl.ds(pl.multiple_of(k * W + a * HALF, HALF), HALF)] = block
        return 0

    lax.fori_loop(0, NQ, lay_table, 0)
    logits[...] = rows_dot(table[...], tok_t[...])

    lg = logits[...]
    top = jnp.max(lg, axis=1, keepdims=True)
    local = jnp.exp(lg - top)
    total = jnp.sum(local, axis=1, keepdims=True)
    lanes = lax.broadcasted_iota(jnp.int32, (S, 128), 1)
    stat[0] = jnp.where(lanes == 0, top, jnp.where(lanes == 1, total, 0.0)).T[0:8]
    raised = jnp.exp(lg - jnp.max(lg, axis=0, keepdims=True))
    comb = raised / jnp.sum(raised, axis=0, keepdims=True)
    weight[...] = comb
    local_b, comb_b = local.astype(BF16), comb.astype(BF16)

    def place(target, a, k, values):
        ky, kl = div(k, XL), rem(k, XL)
        for cc in range(C):
            for hh in range(XH):
                xx = hh * XL + kl
                at = ky * N + xx if a == 0 else xx * N + ky
                row = (cc * XH + hh) * ZR
                target[a, cc, at] = values[row : row + ZR].reshape(Z, 8, values.shape[1]).astype(BF16)

    def partial_sums(k, _):
        span = pl.ds(pl.multiple_of(k * W, W), W)
        place(pb, 0, k, rows_dot(local_b, tok[:, span]))
        place(pb, 1, k, rows_dot(comb_b, og[:, span]))
        return 0

    lax.fori_loop(0, NQ, partial_sums, 0)
    sum_chunk, grad_chunk = end_of(reduce(pb, pb1, pb2, pb3, rbc, rb1, rb2, rbz, True))

    stats = jnp.concatenate([stat[4], jnp.zeros((120, S), F32)], axis=0).T
    factor[...] = stats
    sum_chunk = sum_chunk / factor[pl.ds(own_row, 8), 1:2]
    seq_in[q, 0] = sum_chunk.astype(BF16)
    seq_in[q, 1] = grad_chunk.astype(BF16)
    moves = [send(seq_in.at[q], seq_in.at[q], q_to(i)[1]) for i in range(1, NQ)]
    big[2].wait()
    big[3].wait()
    arrive(moves)
    slot_rows = jnp.concatenate([seq_in[k, 0].astype(F32) for k in range(NQ)], axis=1)
    grad_rows = jnp.concatenate([seq_in[k, 1].astype(F32) for k in range(NQ)], axis=1)
    slot_b, grad_b = slot_rows.astype(BF16), grad_rows.astype(BF16)
    upper = lax.broadcasted_iota(jnp.int32, (8, 1), 0) < 4

    def pick(f, g):
        return jnp.where(upper, f, g)

    pre = pick(rows_dot(slot_b, win[0]), rows_dot(slot_b, win[1]))
    hidden, slope = gelu_and_slope(pre)
    hid_grad = pick(cols_dot(grad_b, wout[0]), cols_dot(grad_b, wout[1]))
    hidden = hidden.astype(BF16)
    act = (hid_grad * slope).astype(BF16)
    out_part = pick(rows_dot(hidden, wout[0]), rows_dot(hidden, wout[1]))
    in_part = pick(cols_dot(act, win[0]), cols_dot(act, win[1]))
    for k in range(NQ):
        seq_out[k, 0] = out_part[:, k * W : (k + 1) * W].astype(BF16)
        seq_out[k, 1] = in_part[:, k * W : (k + 1) * W].astype(BF16)
    moves = []
    for i in range(1, NQ):
        k, device = q_to(i)
        moves.append(send(seq_out.at[k], seq_rec.at[i - 1], device))
    arrive(moves)
    for a in range(2):
        total = seq_out[q, a].astype(F32)
        for i in range(NQ - 1):
            total += seq_rec[i, a].astype(F32)
        gath_d[a, y, xl, c, xh, z] = total.astype(BF16)
    part = jnp.sum(sum_chunk * total.astype(BF16).astype(F32), axis=1, keepdims=True)
    spots = lax.broadcasted_iota(jnp.int32, (8, S), 1)
    cen[0] = jnp.where(spots == own_row + lines, part, 0.0)
    end_of(gather(gath_d, (cen, cen_z, cen_1, cen_2, cen_c)))

    comb_g[...] = jnp.zeros_like(comb_g)
    disp_g[...] = jnp.zeros_like(disp_g)

    def back(k, _):
        span = pl.ds(pl.multiple_of(k * W, W), W)
        ky, kl = div(k, XL), rem(k, XL)
        comb_g[...] += rows_dot(flat(gath_d[0, ky, kl]).astype(BF16), og_t[span, :])
        block = flat(gath_d[1, ky, kl]).astype(BF16)
        grads[:, span] = block
        disp_g[...] += rows_dot(block, tok_t[span, :])
        return 0

    lax.fori_loop(0, NQ, back, 0)
    centre_row = jnp.sum(cen[3] + cen_c[0], axis=0, keepdims=True)
    centre = jnp.broadcast_to(centre_row, (128, S)).T[:, 0:1]
    comb = weight[...]
    comb_grad = comb_g[...]
    disp = jnp.exp(logits[...] - factor[:, 0:1]) / factor[:, 1:2]
    mean = jnp.sum(comb * comb_grad, axis=0, keepdims=True)
    logit_grad = disp * (disp_g[...] - centre) + comb * (comb_grad - mean)
    logit_b = logit_grad.astype(BF16)

    def table_sums(k, _):
        values = rows_dot(logit_b, tok[:, pl.ds(pl.multiple_of(k * W, W), W)])
        for a in range(2):
            place(pg, a, k, values[:, a * HALF : (a + 1) * HALF])
        return 0

    lax.fori_loop(0, NQ, table_sums, 0)
    steps = reduce(pg, pg1, pg2, pg3, rgc, rg1, rg2, rgz, False)
    next(steps)
    both[:, 0:S] = disp.T.astype(BF16)
    both[:, S : 2 * S] = logit_grad.T.astype(BF16)
    next(steps)

    def patch_grads(k, _):
        span = pl.ds(pl.multiple_of(k * W, W), W)
        tg[:, span] = (rows_dot(both[:, 0:S], grads[:, span]) + rows_dot(both[:, S : 2 * S], table[:, span])).astype(BF16)
        return 0

    lax.fori_loop(0, NQ, patch_grads, 0)
    out_copy = pltpu.make_async_copy(tg, tg_hbm, local_sem.at[6])
    out_copy.start()
    parts = end_of(steps)
    for a in range(2):
        sg_out[:, a * HALF : (a + 1) * HALF] = parts[a]
    for copy in begun:
        copy.wait_send()
    out_copy.wait()


def copies_of(sizes):
    Y, XL, Z, XH, C = sizes
    N, NQ = XL * XH, Y * XL
    plain = (Z - 1) + 4 * (N - 1) + 1
    beside = (Z - 1) + 2 * (N - 1) + 1
    return 4 * plain + 2 * beside + 2 * (NQ - 1)


def shards(sizes, tokens, slot_embed, expert_in, expert_out, out_grad):
    Y, XL, Z, XH, C = sizes
    N, NQ = XL * XH, Y * XL
    T, D = tokens.shape
    S = slot_embed.shape[1] * Z * XH * C
    W = D // NQ
    H = W // 2
    vm = pltpu.VMEM

    def reduce_buffers(w):
        return [
            vm((2, C, N * N, Z, 8, w), BF16),
            vm((2, N * N, Z, 8, w), BF16),
            vm((2, N, Z, 8, w), BF16),
            vm((2, Z, 8, w), BF16),
            vm((2, N * N, Z, 8, w), BF16),
            vm((2, N - 1, N, Z, 8, w), BF16),
            vm((2, N - 1, Z, 8, w), BF16),
            vm((Z - 1, 2, 8, w), BF16),
        ]

    n = copies_of(sizes)
    scratch = [
        vm((T, D), BF16), vm((T, D), BF16), vm(expert_in.shape, BF16), vm(expert_out.shape, BF16),
        vm((D, T), BF16), vm((D, T), BF16), vm((S, D), BF16), vm((S, D), BF16),
        vm((S, T), F32), vm((S, T), F32), vm((8, 128), F32), vm((S, T), F32), vm((S, T), F32),
        vm((T, 2 * S), BF16), vm((T, D), BF16), vm((S, 128), F32),
        vm((2, Y, XL, C, XH, Z, 8, H), BF16), vm((2, Y, XL, C, XH, Z, 8, W), BF16),
        *reduce_buffers(W), *reduce_buffers(H),
        vm((5, 8, S), F32), vm((1, 8, S), F32), vm((N - 1, 8, S), F32), vm((N - 1, 8, S), F32), vm((Z - 1, 8, S), F32),
        vm((4, 8, S), F32), vm((Z - 1, 8, S), F32), vm((N - 1, 8, S), F32), vm((N - 1, 8, S), F32), vm((1, 8, S), F32),
        vm((NQ, 2, 8, W), BF16), vm((NQ, 2, 8, W), BF16), vm((NQ - 1, 2, 8, W), BF16),
        pltpu.SemaphoreType.DMA((7,)), pltpu.SemaphoreType.DMA((n,)), pltpu.SemaphoreType.DMA((n,)),
    ]
    hbm = pl.BlockSpec(memory_space=pl.ANY)
    tok_grad, slot_grad = pl.pallas_call(
        functools.partial(kernel, sizes),
        out_shape=(jax.ShapeDtypeStruct((T, D), BF16), jax.ShapeDtypeStruct((8, W), F32)),
        in_specs=[hbm] * 5,
        out_specs=(hbm, pl.BlockSpec(memory_space=pltpu.VMEM)),
        scratch_shapes=scratch,
        compiler_params=pltpu.CompilerParams(collective_id=0, has_side_effects=True),
        name="soft_moe",
    )(tokens, slot_embed.T, expert_in, expert_out, out_grad)
    return tok_grad, slot_grad.T


SIZES = (4, 2, 8, 2, 2)


def solution(mesh, sizes=SIZES):
    torus = Mesh(mesh.devices.reshape(sizes), AXES)
    placed = (
        P(SEQ_EXP, None),
        P(None, EXP),
        P(EXP, None, SEQ),
        P(EXP, SEQ, None),
        P(SEQ_EXP, None),
    )
    return jax.shard_map(
        functools.partial(shards, sizes),
        mesh=torus,
        in_specs=placed,
        out_specs=(P(SEQ_EXP, None), P(SEQ, EXP)),
        check_vma=False,
    )
```

```python
import functools

import jax
import jax.numpy as jnp
from jax import lax
from jax.experimental import pallas as pl
from jax.experimental.pallas import tpu as pltpu
from jax.sharding import Mesh
from jax.sharding import PartitionSpec as P

EXP = ("exp_0", "exp_1", "exp_2")
SEQ = ("seq_0", "seq_1")
SEQ_EXP = ("seq_0", "seq_1", "exp_0", "exp_1", "exp_2")
AXES = SEQ_EXP
F32, BF16 = jnp.float32, jnp.bfloat16
ROOT = 0.7978845608028654


def rows_dot(left, right):
    return lax.dot_general(left, right, (((1,), (0,)), ((), ())), preferred_element_type=F32)


def cols_dot(left, right):
    return lax.dot_general(left, right, (((1,), (1,)), ((), ())), preferred_element_type=F32)


def gelu_and_slope(v):
    t = jnp.tanh(ROOT * (v + 0.044715 * (v * v * v)))
    value = 0.5 * v * (1.0 + t)
    slope = 0.5 * (1.0 + t) + 0.5 * v * (1.0 - t * t) * (ROOT * (1.0 + 3.0 * 0.044715 * (v * v)))
    return value, slope


def flat(block):
    block = block.astype(F32)
    return block.reshape(-1, block.shape[-1])


def kernel(
    sizes,
    tok_hbm, slot_hbm, win_hbm, wout_hbm, og_hbm,
    tg, sg_out,
    tok, og, win, wout, tok_t, og_t, pair, logits, weight, comb_g, disp_g, both, tg_send, tg_rec,
    gath_a, gath_d,
    pb, pb2, pb3, rb1, rb2, rbz,
    pg, pg2, pg3, rg1, rg2, rgz,
    stat, stat_1, stat_2, stat_z, factor,
    cen, cen_z, cen_1, cen_2,
    seq_in, seq_out, seq_rec, line, line_rec,
    local_sem, send_sem, recv_sem,
):
    Y, XL, Z, XH, C = sizes
    N, NQ = XL * XH, Y * XL
    assert Y == N and C == 2 and XL == 2 and XH == 2
    S = XH * Z * 8
    T = tok.shape[0] // 2
    W = tok.shape[1] // NQ
    HALF = W // 2
    ZR = Z * 8
    y, xl, z, xh, c = (lax.axis_index(name) for name in AXES)
    x, q = xh * XL + xl, y * XL + xl
    rem, div = lax.rem, lax.div

    def z_to(i):
        k = rem(z + i, Z)
        return k, {"exp_0": k}

    def y_to(i):
        k = rem(y + i, N)
        return k, {"seq_0": k}

    def x_to(i):
        k = rem(x + i, N)
        return k, {"exp_1": div(k, XL), "seq_1": rem(k, XL)}

    def seq_to(dy, dl):
        ky, kl = rem(y + dy, N), rem(xl + dl, XL)
        return ky * XL + kl, {"seq_0": ky, "seq_1": kl}

    def seq_from(dy, dl):
        return rem(y + N - dy, N) * XL + rem(xl + dl, XL)

    def by_x(k):
        return rem(k, XL) * Y + div(k, XL)

    other = {"exp_2": 1 - c}
    far_first = (2, 1, 3)
    seq_far_first = ((2, 1), (2, 0), (1, 1), (3, 1), (1, 0), (3, 0), (0, 1))
    MESH = pl.DeviceIdType.MESH
    count = [0]
    begun = []

    def send(src, dst, device):
        k = count[0]
        count[0] += 1
        copy = pltpu.make_async_remote_copy(
            src_ref=src, dst_ref=dst, send_sem=send_sem.at[k], recv_sem=recv_sem.at[k],
            device_id=device, device_id_type=MESH,
        )
        copy.start()
        begun.append(copy)
        return copy

    def arrive(copies):
        for copy in copies:
            copy.wait_recv()

    def columns(k, width):
        return pl.ds(pl.multiple_of(k * width, width), width)

    mine, theirs = pl.ds(0, T), pl.ds(T, T)
    first = [
        pltpu.make_async_copy(
            slot_hbm.at[:, columns(start, HALF)],
            gath_a.at[a, y, xl, xh, z],
            local_sem.at[a],
        )
        for a, start in ((0, y * XL + xl), (1, NQ + xl * Y + y))
    ]
    big = [
        pltpu.make_async_copy(src, dst, local_sem.at[2 + k])
        for k, (src, dst) in enumerate(
            ((tok_hbm, tok.at[mine]), (og_hbm, og.at[mine]), (win_hbm, win), (wout_hbm, wout))
        )
    ]
    for copy in first + big:
        copy.start()

    barrier = pltpu.get_barrier_semaphore()
    partners = [z_to(i)[1] for i in range(1, Z)]
    partners += [y_to(i)[1] for i in range(1, N)]
    partners += [x_to(i)[1] for i in range(1, N)]
    partners += [seq_to(*step)[1] for step in seq_far_first]
    partners += [other]
    for device in partners:
        pl.semaphore_signal(barrier, inc=1, device_id=device, device_id_type=MESH)
    for copy in first:
        copy.wait()
    pl.semaphore_wait(barrier, len(partners))

    def gather(buf, beside=None):
        moves = [send(buf.at[:, y, xl, xh, z], buf.at[:, y, xl, xh, z], z_to(i)[1]) for i in (4, 3, 5, 2, 6, 1, 7) if i < Z]
        if beside:
            own, over_z, over_1, over_2 = beside
            moves += [send(own.at[0], over_z.at[i - 1], z_to(i)[1]) for i in range(1, Z)]
        yield
        arrive(moves)
        moves = []
        for i in far_first:
            moves.append(send(buf.at[0, y, xl, xh], buf.at[0, y, xl, xh], x_to(i)[1]))
            moves.append(send(buf.at[1, y, xl, xh], buf.at[1, y, xl, xh], y_to(i)[1]))
        if beside:
            total = own[0]
            for i in range(1, Z):
                total += over_z[i - 1]
            own[1] = total
            moves += [send(own.at[1], over_1.at[i - 1], x_to(i)[1]) for i in range(1, N)]
        yield
        arrive(moves)
        moves = {}
        for i in far_first:
            moves[0, i] = [send(buf.at[0, y], buf.at[0, y], y_to(i)[1])]
            moves[1, i] = [send(buf.at[1, :, xl, xh], buf.at[1, :, xl, xh], x_to(i)[1])]
        if beside:
            total = own[1]
            for i in range(1, N):
                total += over_1[i - 1]
            own[2] = total
            moves[2, 0] = [send(own.at[2], over_2.at[i - 1], y_to(i)[1]) for i in range(1, N)]
        yield moves

    lines = lax.broadcasted_iota(jnp.int32, (8, S), 0)

    def merge(entries, k):
        top = entries[0][0:1]
        for entry in entries[1:]:
            top = jnp.maximum(top, entry[0:1])
        scales = [jnp.exp(entry[0:1] - top) for entry in entries]
        total = entries[0][1:2] * scales[0]
        for entry, scale in zip(entries[1:], scales[1:]):
            total += entry[1:2] * scale
        turned = jnp.zeros((8, S), F32)
        for j, scale in enumerate(scales):
            turned = jnp.where(lines == j, scale, turned)
        factor[k] = jnp.concatenate([turned, jnp.zeros((120, S), F32)], axis=0).T
        return jnp.where(lines == 0, top, jnp.where(lines == 1, total, 0.0))

    def joined(parts, scale, row, rows):
        total = None
        for k, part in enumerate(parts):
            part = flat(part)
            if scale is not None:
                part = part * factor[scale, pl.ds(pl.multiple_of(row, 8), rows), k : k + 1]
            total = part if total is None else total + part
        return total

    def reduce(p, s2, s3, r1, r2, rz, moves, stats=None):
        w = p.shape[-1]
        scaled = stats is not None
        if scaled:
            arrive(stats)
            stat[1] = merge([stat[0]] + [stat_1[i] for i in range(N - 1)], 0)
            stats = [send(stat.at[1], stat_2.at[i - 1], x_to(i)[1]) for i in far_first]
        arrive(moves)

        def second_sum(b, _):
            for a, me in ((0, y), (1, x)):
                parts = [p[a, me, b]] + [r1[a, i, b] for i in range(N - 1)]
                total = joined(parts, 0 if scaled and a == 0 else None, div(b, XL) * ZR, ZR)
                s2[a, b] = total.reshape(Z, 8, w).astype(BF16)
            return 0

        lax.fori_loop(0, N, second_sum, 0)
        moves = []
        for i in far_first:
            k, device = x_to(i)
            moves.append(send(s2.at[0, k], r2.at[0, i - 1], device))
            k, device = y_to(i)
            moves.append(send(s2.at[1, k], r2.at[1, i - 1], device))
        yield
        if scaled:
            arrive(stats)
            stat[2] = merge([stat[1]] + [stat_2[i] for i in range(N - 1)], 1)
            stats = [send(stat.at[2], stat_z.at[i - 1], z_to(i)[1]) for i in range(1, Z)]
        arrive(moves)
        for a, me in ((0, x), (1, y)):
            parts = [s2[a, me]] + [r2[a, i] for i in range(N - 1)]
            total = joined(parts, 1 if scaled and a == 0 else None, xh * ZR, ZR)
            s3[a] = total.reshape(Z, 8, w).astype(BF16)
        moves = []
        for i in (4, 3, 5, 2, 6, 1, 7):
            if i < Z:
                k, device = z_to(i)
                moves.append(send(s3.at[:, k], rz.at[i - 1], device))
        if scaled:
            arrive(stats)
            final = merge([stat[2]] + [stat_z[i] for i in range(Z - 1)], 2)
            factor[3] = jnp.concatenate([final, jnp.zeros((120, S), F32)], axis=0).T
        yield
        arrive(moves)
        result = []
        for a in range(2):
            parts = [s3[a, z]] + [rz[i, a] for i in range(Z - 1)]
            result.append(joined(parts, 2 if scaled and a == 0 else None, own_row, 8))
        yield result

    def end_of(steps):
        last = None
        for last in steps:
            pass
        return last

    own_row = pl.multiple_of(xh * ZR + z * 8, 8)

    def turn(source, target, half):
        target[:, half * T : half * T + T] = source[half * T : half * T + T].T

    steps = gather(gath_a)
    next(steps)
    swaps = [send(tok_hbm, tok.at[theirs], other)]
    big[0].wait()
    turn(tok, tok_t, 0)
    next(steps)
    swaps.append(send(og_hbm, og.at[theirs], other))
    arrive(swaps[:1])
    turn(tok, tok_t, 1)
    last = next(steps)
    logits[...] = jnp.zeros_like(logits)

    def table_by_y(ky):
        span = columns(ky, XL * HALF)
        block = jnp.concatenate([flat(gath_a[0, ky, kl]) for kl in range(XL)], axis=1).astype(BF16)
        pair[S : 2 * S, span] = block
        logits[...] += rows_dot(block, tok_t[span, :])

    def table_by_x(kx):
        kh, kl = div(kx, XL), rem(kx, XL)
        span = pl.ds(pl.multiple_of(NQ * HALF + kl * (Y * HALF), HALF), Y * HALF)
        block = jnp.concatenate([flat(gath_a[1, ky, kl, kh]) for ky in range(Y)], axis=1).astype(BF16)
        pair[pl.ds(pl.multiple_of(S + kh * ZR, ZR), ZR), span] = block
        logits[columns(kh, ZR), :] += rows_dot(block, tok_t[span, :])

    big[1].wait()
    turn(og, og_t, 0)
    arrive(swaps[1:])
    turn(og, og_t, 1)
    table_by_y(y)
    table_by_x(x)
    for i in (1, 3, 2):
        arrive(last[0, i])
        table_by_y(rem(y + N - i, N))
        arrive(last[1, i])
        table_by_x(rem(x + N - i, N))
    lg = logits[...]

    slots_b = jnp.max(lg, axis=0, keepdims=True)
    raised = jnp.exp(lg - slots_b)
    sums_b = jnp.sum(raised, axis=0, keepdims=True)
    wide = lax.broadcasted_iota(jnp.int32, (8, 2 * T), 0)
    line[0] = jnp.where(wide == 0, slots_b, sums_b)
    line_move = send(line.at[0], line_rec.at[0], other)
    top = jnp.max(lg, axis=1, keepdims=True)
    local = jnp.exp(lg - top)
    total = jnp.sum(local, axis=1, keepdims=True)
    lanes = lax.broadcasted_iota(jnp.int32, (S, 128), 1)
    stat[0] = jnp.where(lanes == 0, top, jnp.where(lanes == 1, total, 0.0)).T[0:8]
    stats = [send(stat.at[0], stat_1.at[i - 1], y_to(i)[1]) for i in far_first]
    local_b = local.astype(BF16)

    def place(target, a, ky, kl, values):
        for hh in range(XH):
            block = values[hh * ZR : hh * ZR + ZR].reshape(Z, 8, values.shape[1]).astype(BF16)
            if a == 0:
                target[0, ky, hh * XL + kl] = block
            else:
                target[1, hh * XL + kl, ky] = block

    moves = []
    for i in far_first + (0,):
        ky, device = y_to(i)

        values = rows_dot(local_b, tok[:, columns(ky, XL * W)])
        for kl in range(XL):
            place(pb, 0, ky, kl, values[:, kl * W : (kl + 1) * W])
        if i:
            moves.append(send(pb.at[0, ky], rb1.at[0, i - 1], device))
        if i == 1:
            arrive([line_move])
            got = line_rec[0]
            got = jnp.concatenate([got[:, T:], got[:, :T]], axis=1)
            high = jnp.maximum(slots_b, got[0:1])
            low = jnp.exp(slots_b - high)
            share = low / (sums_b * low + got[1:2] * jnp.exp(got[0:1] - high))
            comb = raised * share
            weight[...] = comb
            comb_b = comb.astype(BF16)
    for near in (0, 1):
        kl = rem(xl + near, XL)

        for pick_y in range(Y // 2):
            values = rows_dot(comb_b, og[:, columns(kl * (Y // 2) + pick_y, 2 * W)])
            for k in range(2):
                place(pb, 1, 2 * pick_y + k, kl, values[:, k * W : (k + 1) * W])
        for i in (1, 3) if near else (2,):
            k, device = x_to(i)
            moves.append(send(pb.at[1, k], rb1.at[1, i - 1], device))
    sum_chunk, grad_chunk = end_of(reduce(pb, pb2, pb3, rb1, rb2, rbz, moves, stats))

    sum_chunk = sum_chunk / factor[3, pl.ds(own_row, 8), 1:2]
    seq_in[q, 0] = sum_chunk.astype(BF16)
    seq_in[q, 1] = grad_chunk.astype(BF16)
    moves = {step: send(seq_in.at[q], seq_in.at[q], seq_to(*step)[1]) for step in seq_far_first}
    big[2].wait()
    big[3].wait()
    upper = lax.broadcasted_iota(jnp.int32, (8, 1), 0) < 4

    def pick(f, g):
        return jnp.where(upper, f, g)

    pre = hid_grad = None
    for step in ((0, 0),) + seq_far_first[::-1]:
        if step != (0, 0):
            arrive([moves[step]])
        k = seq_from(*step)
        slot_b, grad_b = (seq_in[k, a].astype(F32).astype(BF16) for a in range(2))
        more = [rows_dot(slot_b, win[e, columns(k, W), :]) for e in range(2)]
        pre = more if pre is None else [f + g for f, g in zip(pre, more)]
        more = [cols_dot(grad_b, wout[e, :, columns(by_x(k), W)]) for e in range(2)]
        hid_grad = more if hid_grad is None else [f + g for f, g in zip(hid_grad, more)]
    hidden, slope = gelu_and_slope(pick(*pre))
    hidden = hidden.astype(BF16)
    act = (pick(*hid_grad) * slope).astype(BF16)
    moves = []
    for step in seq_far_first + ((0, 0),):
        k, device = seq_to(*step)
        in_part = pick(*(cols_dot(act, win[e, columns(k, W), :]) for e in range(2)))
        out_part = pick(*(rows_dot(hidden, wout[e, :, columns(by_x(k), W)]) for e in range(2)))
        seq_out[k, 0] = in_part.astype(BF16)
        seq_out[k, 1] = out_part.astype(BF16)
        if step != (0, 0):
            moves.append(send(seq_out.at[k], seq_rec.at[step[0] * XL + step[1] - 1], device))
    arrive(moves)
    for a in (1, 0):
        total = seq_out[q, a].astype(F32)
        for i in range(NQ - 1):
            total += seq_rec[i, a].astype(F32)
        gath_d[a, y, xl, xh, z] = total.astype(BF16)
    part = jnp.sum(sum_chunk * total.astype(BF16).astype(F32), axis=1, keepdims=True)
    spots = lax.broadcasted_iota(jnp.int32, (8, S), 1)
    cen[0] = jnp.where(spots == own_row + lines, part, 0.0)
    *_, last = gather(gath_d, (cen, cen_z, cen_1, cen_2))

    comb_g[...] = jnp.zeros_like(comb_g)
    disp_g[...] = jnp.zeros_like(disp_g)

    def back_disp(ky):
        span = columns(ky, XL * W)
        block = jnp.concatenate([flat(gath_d[0, ky, kl]) for kl in range(XL)], axis=1).astype(BF16)
        pair[0:S, span] = block
        disp_g[...] += rows_dot(block, tok_t[span, :])

    def back_comb(kx):
        kh, kl = div(kx, XL), rem(kx, XL)
        block = jnp.concatenate([flat(gath_d[1, ky, kl, kh]) for ky in range(Y)], axis=1).astype(BF16)
        comb_g[columns(kh, ZR), :] += rows_dot(block, og_t[columns(kl, Y * W), :])

    back_comb(x)
    back_disp(y)
    for i in (1, 3, 2):
        arrive(last[1, i])
        back_comb(rem(x + N - i, N))
        if i == 2:
            comb = weight[...]
            comb_grad = comb_g[...]
            mean = jnp.sum(comb * comb_grad, axis=0, keepdims=True)
            line[1] = jnp.broadcast_to(mean, (8, 2 * T))
            line_move = send(line.at[1], line_rec.at[1], other)
        arrive(last[0, i])
        back_disp(rem(y + N - i, N))
    arrive(last[2, 0])
    centre_row = cen[2]
    for i in range(N - 1):
        centre_row += cen_2[i]
    centre = jnp.broadcast_to(jnp.sum(centre_row, axis=0, keepdims=True), (128, S)).T[:, 0:1]
    disp = jnp.exp(logits[...] - factor[3, :, 0:1]) / factor[3, :, 1:2]
    disp_part = disp * (disp_g[...] - centre)
    arrive([line_move])
    got = line_rec[1]
    mean = mean + jnp.concatenate([got[:, T:], got[:, :T]], axis=1)[0:1]
    logit_grad = disp_part + comb * (comb_grad - mean)
    logit_b = logit_grad.astype(BF16)

    moves = []
    for i in far_first + (0,):
        ky, device = y_to(i)

        values = rows_dot(logit_b, tok[:, columns(ky, XL * W)])
        for kl in range(XL):
            for a in range(2):
                place(pg, a, ky, kl, values[:, (2 * kl + a) * HALF : (2 * kl + a + 1) * HALF])
        if i:
            moves.append(send(pg.at[0, ky], rg1.at[0, i - 1], device))
    for i in far_first:
        k, device = x_to(i)
        moves.append(send(pg.at[1, k], rg1.at[1, i - 1], device))
    both[:, 0:S] = disp.T.astype(BF16)
    both[:, S : 2 * S] = logit_grad.T.astype(BF16)

    def their_grads(k, _):
        tg_send[:, columns(k, W)] = rows_dot(both[T : 2 * T], pair[:, columns(k, W)]).astype(BF16)
        return 0

    lax.fori_loop(0, NQ, their_grads, 0)
    tg_move = send(tg_send, tg_rec, other)
    steps = reduce(pg, pg2, pg3, rg1, rg2, rgz, moves)
    next(steps)
    arrive([tg_move])

    def own_grads(k, _):
        span = columns(k, W)
        tg[:, span] = (rows_dot(both[0:T], pair[:, span]) + tg_rec[:, span].astype(F32)).astype(BF16)
        return 0

    lax.fori_loop(0, NQ, own_grads, 0)
    parts = end_of(steps)
    for a in range(2):
        sg_out[:, a * HALF : (a + 1) * HALF] = parts[a]
    for copy in begun:
        copy.wait_send()


def copies_of(sizes):
    Y, XL, Z, XH, C = sizes
    N, NQ = XL * XH, Y * XL
    return 4 * (Z - 1 + 4 * (N - 1)) + 2 * (Z - 1 + 2 * (N - 1)) + 2 * (NQ - 1) + 5


def shards(sizes, tokens, slot_embed, expert_in, expert_out, out_grad):
    Y, XL, Z, XH, C = sizes
    N, NQ = XL * XH, Y * XL
    T, D = tokens.shape
    S = slot_embed.shape[1] * Z * XH
    W = D // NQ
    H = W // 2
    vm = pltpu.VMEM

    def reduce_buffers(w):
        return [
            vm((2, N, N, Z, 8, w), BF16),
            vm((2, N, Z, 8, w), BF16),
            vm((2, Z, 8, w), BF16),
            vm((2, N - 1, N, Z, 8, w), BF16),
            vm((2, N - 1, Z, 8, w), BF16),
            vm((Z - 1, 2, 8, w), BF16),
        ]

    n = copies_of(sizes)
    scratch = [
        vm((2 * T, D), BF16), vm((2 * T, D), BF16), vm(expert_in.shape, BF16), vm(expert_out.shape, BF16),
        vm((D, 2 * T), BF16), vm((D, 2 * T), BF16), vm((2 * S, D), BF16),
        vm((S, 2 * T), F32), vm((S, 2 * T), F32), vm((S, 2 * T), F32), vm((S, 2 * T), F32),
        vm((2 * T, 2 * S), BF16), vm((T, D), BF16), vm((T, D), BF16),
        vm((2, Y, XL, XH, Z, 8, H), BF16), vm((2, Y, XL, XH, Z, 8, W), BF16),
        *reduce_buffers(W), *reduce_buffers(H),
        vm((3, 8, S), F32), vm((N - 1, 8, S), F32), vm((N - 1, 8, S), F32), vm((Z - 1, 8, S), F32), vm((4, S, 128), F32),
        vm((3, 8, S), F32), vm((Z - 1, 8, S), F32), vm((N - 1, 8, S), F32), vm((N - 1, 8, S), F32),
        vm((NQ, 2, 8, W), BF16), vm((NQ, 2, 8, W), BF16), vm((NQ - 1, 2, 8, W), BF16),
        vm((2, 8, 2 * T), F32), vm((2, 8, 2 * T), F32),
        pltpu.SemaphoreType.DMA((6,)), pltpu.SemaphoreType.DMA((n,)), pltpu.SemaphoreType.DMA((n,)),
    ]
    hbm = pl.BlockSpec(memory_space=pl.ANY)
    tok_grad, slot_grad = pl.pallas_call(
        functools.partial(kernel, sizes),
        out_shape=(pltpu.VMEM((T, D), BF16), pltpu.VMEM((8, W), F32)),
        in_specs=[hbm] * 5,
        out_specs=(pl.BlockSpec(memory_space=pltpu.VMEM), pl.BlockSpec(memory_space=pltpu.VMEM)),
        scratch_shapes=scratch,
        compiler_params=pltpu.CompilerParams(collective_id=0, has_side_effects=True),
        name="soft_moe",
    )(tokens, slot_embed.T, expert_in, expert_out, out_grad)
    return tok_grad, slot_grad.T


SIZES = (4, 2, 8, 2, 2)


def solution(mesh, sizes=SIZES):
    torus = Mesh(mesh.devices.reshape(sizes), AXES)
    placed = (
        P(SEQ_EXP, None),
        P(None, EXP),
        P(EXP, None, SEQ),
        P(EXP, SEQ, None),
        P(SEQ_EXP, None),
    )
    return jax.shard_map(
        functools.partial(shards, sizes),
        mesh=torus,
        in_specs=placed,
        out_specs=(P(SEQ_EXP, None), P(SEQ, EXP)),
        check_vma=False,
    )
```

```python
import functools

import jax
import jax.numpy as jnp
from jax import lax
from jax.experimental import pallas as pl
from jax.experimental.pallas import tpu as pltpu
from jax.sharding import Mesh
from jax.sharding import PartitionSpec as P

EXP = ("exp_0", "exp_1", "exp_2")
SEQ = ("seq_0", "seq_1")
SEQ_EXP = ("seq_0", "seq_1", "exp_0", "exp_1", "exp_2")
AXES = SEQ_EXP
F32, BF16 = jnp.float32, jnp.bfloat16
ROOT = 0.7978845608028654


def rows_dot(left, right):
    return lax.dot_general(left, right, (((1,), (0,)), ((), ())), preferred_element_type=F32)


def cols_dot(left, right):
    return lax.dot_general(left, right, (((1,), (1,)), ((), ())), preferred_element_type=F32)


def gelu_and_slope(v):
    t = jnp.tanh(ROOT * (v + 0.044715 * (v * v * v)))
    value = 0.5 * v * (1.0 + t)
    slope = 0.5 * (1.0 + t) + 0.5 * v * (1.0 - t * t) * (ROOT * (1.0 + 3.0 * 0.044715 * (v * v)))
    return value, slope


def flat(block):
    block = block.astype(F32)
    return block.reshape(-1, block.shape[-1])


def kernel(
    sizes,
    tok_hbm, slot_hbm, win_hbm, wout_hbm, og_hbm,
    tg, sg_out,
    tok, og, win, wout, tok_t, og_t, pair, logits, weight, comb_g, disp_g, both, tg_send, tg_rec,
    own_a, own_d, gath_a, gath_d,
    pb, pb2, pb3, rb1, rb2, rbz,
    pg, pg2, pg3, rg1, rg2, rgz,
    stat, stat_p, stat_z, factor, scale_out, scale_in,
    cen, cen_z, cen_p,
    seq_in, seq_out, seq_rec, line, line_rec,
    local_sem, send_sem, recv_sem,
):
    Y, XL, Z, XH, C = sizes
    N, NQ = XL * XH, Y * XL
    assert Y == N and C == 2 and XL == 2 and XH == 2
    S = XH * Z * 8
    T = tok.shape[0] // 2
    W = tok.shape[1] // NQ
    HALF = W // 2
    ZR = Z * 8
    y, xl, z, xh, c = (lax.axis_index(name) for name in AXES)
    x, q = xh * XL + xl, y * XL + xl
    rem, div = lax.rem, lax.div

    def z_to(i):
        k = rem(z + i, Z)
        return k, {"exp_0": k}

    def owner_to(i):
        k = rem(z + i, Z)
        return k, {"exp_0": k, "exp_2": 1 - c}

    def y_to(i):
        k = rem(y + i, N)
        return k, {"seq_0": k}

    def x_to(i):
        k = rem(x + i, N)
        return k, {"exp_1": div(k, XL), "seq_1": rem(k, XL)}

    def plane_to(dy, dx):
        kx = rem(x + dx, N)
        return {"seq_0": rem(y + dy, N), "exp_1": div(kx, XL), "seq_1": rem(kx, XL)}

    def seq_to(dy, dl):
        ky, kl = rem(y + dy, N), rem(xl + dl, XL)
        return ky * XL + kl, {"seq_0": ky, "seq_1": kl}

    def seq_from(dy, dl):
        return rem(y + N - dy, N) * XL + rem(xl + dl, XL)

    def by_x(k):
        return rem(k, XL) * Y + div(k, XL)

    other = {"exp_2": 1 - c}
    far_first = (2, 1, 3)
    z_far_first = sorted(range(Z), key=lambda i: -min(i, Z - i))
    plane = [(dy, dx) for dy in (2, 1, 3, 0) for dx in (2, 1, 3, 0) if dy or dx]
    seq_far_first = ((2, 1), (2, 0), (1, 1), (3, 1), (1, 0), (3, 0), (0, 1))
    MESH = pl.DeviceIdType.MESH
    groups, over = [], [0]

    def group(whole):
        groups.append(whole)
        return len(groups) - 1

    def send(k, src, dst, device):
        pltpu.make_async_remote_copy(
            src_ref=src, dst_ref=dst, send_sem=send_sem.at[k], recv_sem=recv_sem.at[k],
            device_id=device, device_id_type=MESH,
        ).start()

    def arrive(*which):
        for k in which:
            pltpu.make_async_copy(groups[k], groups[k], recv_sem.at[k]).wait()

    def sent(n):
        for k in range(over[0], n):
            pltpu.make_async_copy(groups[k], groups[k], send_sem.at[k]).wait()
        over[0] = max(n, over[0])

    def columns(k, width):
        return pl.ds(pl.multiple_of(k * width, width), width)

    mine, theirs = pl.ds(0, T), pl.ds(T, T)
    first = [
        pltpu.make_async_copy(
            slot_hbm.at[:, columns(start, HALF)],
            own_a.at[a],
            local_sem.at[a],
        )
        for a, start in ((0, y * XL + xl), (1, NQ + xl * Y + y))
    ]
    big = [
        pltpu.make_async_copy(src, dst, local_sem.at[2 + k])
        for k, (src, dst) in enumerate(
            ((tok_hbm, tok.at[mine]), (og_hbm, og.at[mine]), (win_hbm, win), (wout_hbm, wout))
        )
    ]
    for copy in first + big:
        copy.start()

    barrier = pltpu.get_barrier_semaphore()
    partners = [z_to(i)[1] for i in range(1, Z)] + [owner_to(i)[1] for i in range(1, Z)]
    partners += [plane_to(*step) for step in plane]
    partners += [other]
    for device in partners:
        pl.semaphore_signal(barrier, inc=1, device_id=device, device_id_type=MESH)
    for copy in first:
        copy.wait()
    pl.semaphore_wait(barrier, len(partners))

    def gather(block, buf, beside=None):
        along = [group(buf.at[:, y, xl, xh])]
        for i in z_far_first:
            send(along[0], block, buf.at[:, y, xl, xh, z], owner_to(i)[1])
        if beside:
            own, over_z, over_plane = beside
            along.append(group(over_z))
            for i in z_far_first:
                send(along[1], own.at[0], over_z.at[i], owner_to(i)[1])
        yield
        arrive(*along)
        hops = {}
        for i in far_first:
            hops[i] = group(buf.at[:, y, xl, xh])
            send(hops[i], buf.at[0, y, xl, xh], buf.at[0, y, xl, xh], x_to(i)[1])
            send(hops[i], buf.at[1, y, xl, xh], buf.at[1, y, xl, xh], y_to(i)[1])
        last = [group(buf.at[:, 0 : N - 1])]

        def pass_on(j):
            kx = rem(x + N - j, N)
            part = buf.at[0, y, rem(kx, XL), div(kx, XL)]
            for i in far_first:
                send(last[0], part, part, y_to(i)[1])
            part = buf.at[1, rem(y + N - j, N), xl, xh]
            for i in far_first:
                send(last[0], part, part, x_to(i)[1])

        pass_on(0)
        if beside:
            total = over_z[0]
            for i in range(1, Z):
                total += over_z[i]
            own[1] = total
            last.append(group(over_plane))
            for n, step in enumerate(plane):
                send(last[1], own.at[1], over_plane.at[n], plane_to(*step))
        yield
        for j in (1, 3, 2):
            arrive(hops[j])
            pass_on(j)
        yield last

    lines = lax.broadcasted_iota(jnp.int32, (8, S), 0)

    def merge(entries):
        top = entries[0][0]
        for entry in entries[1:]:
            top = jnp.maximum(top, entry[0])
        scales = [jnp.exp(entry[0] - top) for entry in entries]
        total = entries[0][1] * scales[0]
        for entry, scale in zip(entries[1:], scales[1:]):
            total += entry[1] * scale
        return (top, total), scales

    def upright(rows):
        turned = jnp.zeros((16, S), F32)
        tall = lax.broadcasted_iota(jnp.int32, (16, S), 0)
        for k, row in enumerate(rows):
            turned = jnp.where(tall == k, row, turned)
        return jnp.concatenate([turned, jnp.zeros((112, S), F32)], axis=0).T

    def joined(parts, scale, row, rows):
        total = None
        for k, part in enumerate(parts):
            part = flat(part)
            if scale is not None:
                part = part * scale[pl.ds(pl.multiple_of(row, 8), rows), k : k + 1]
            total = part if total is None else total + part
        return total

    def reduce(p, s2, s3, r1, r2, rz, moves, stats=None):
        w = p.shape[-1]
        scaled = stats is not None
        if scaled:
            arrive(*stats)
            stat_of = {(0, 0): stat[0]}
            for n, step in enumerate(plane):
                stat_of[step] = stat_p[n]
            by_y = [merge([(e[0:1], e[1:2]) for e in (stat_of[i, j] for i in range(N))]) for j in range(N)]
            merged, across = merge([joint for joint, _ in by_y])
            stat[1] = jnp.where(lines == 0, merged[0], merged[1])
            stats = [group(stat_z)]
            for i in z_far_first:
                if i:
                    send(stats[0], stat.at[1], stat_z.at[i - 1], z_to(i)[1])
            factor[0] = upright(by_y[0][1])
            factor[1] = upright(across)
        later = [group(r2)]
        for j in far_first + (0,):
            for a, me, (b, device) in ((0, y, x_to(j)), (1, x, y_to(j))):
                arrive(moves[a, j])
                parts = [p[a, me, b]] + [r1[a, i, b] for i in range(N - 1)]
                total = joined(parts, factor.at[0] if scaled and a == 0 else None, div(b, XL) * ZR, ZR)
                s2[a, b] = total.reshape(Z, 8, w).astype(BF16)
                if j:
                    send(later[0], s2.at[a, b], r2.at[a, j - 1], device)
        moves = later
        yield
        if scaled:
            arrive(*stats)
            entries = [stat[1]] + [stat_z[i] for i in range(Z - 1)]
            merged, across = merge([(e[0:1], e[1:2]) for e in entries])
            scale_out[...] = upright(across + list(merged))
            scale_move = group(scale_in)
            send(scale_move, scale_out, scale_in, other)
        arrive(*moves)
        for a, me in ((0, x), (1, y)):
            parts = [s2[a, me]] + [r2[a, i] for i in range(N - 1)]
            total = joined(parts, factor.at[1] if scaled and a == 0 else None, xh * ZR, ZR)
            s3[a] = total.reshape(Z, 8, w).astype(BF16)
        moves = [group(rz)]
        for i in z_far_first:
            k, device = owner_to(i)
            send(moves[0], s3.at[:, k], rz.at[i], device)
        if scaled:
            moves.append(scale_move)
        yield
        arrive(*moves)
        result = []
        for a in range(2):
            parts = [rz[i, a] for i in range(Z)]
            result.append(joined(parts, scale_in if scaled and a == 0 else None, own_row, 8))
        yield result

    def spread(p, r1, a):
        first_to, then_to = (y_to, x_to) if a == 0 else (x_to, y_to)
        moves = {}
        for j in far_first + (0,):
            b = then_to(j)[0]
            moves[a, j] = group(r1.at[a, :, b])
            for i in far_first:
                k, device = first_to(i)
                send(moves[a, j], p.at[a, k, b], r1.at[a, i - 1, b], device)
        return moves

    def end_of(steps):
        last = None
        for last in steps:
            pass
        return last

    own_row = pl.multiple_of(xh * ZR + z * 8, 8)

    def turn(source, target, half):
        target[:, half * T : half * T + T] = source[half * T : half * T + T].T

    steps = gather(own_a, gath_a)
    next(steps)
    swaps = [group(tok.at[theirs]), group(og.at[theirs])]
    send(swaps[0], tok_hbm, tok.at[theirs], other)
    big[0].wait()
    turn(tok, tok_t, 0)
    next(steps)
    send(swaps[1], og_hbm, og.at[theirs], other)
    arrive(swaps[0])
    turn(tok, tok_t, 1)
    last = next(steps)
    logits[...] = jnp.zeros_like(logits)

    def table_by_y(ky):
        span = columns(ky, XL * HALF)
        block = jnp.concatenate([flat(gath_a[0, ky, kl]) for kl in range(XL)], axis=1).astype(BF16)
        pair[S : 2 * S, span] = block
        logits[...] += rows_dot(block, tok_t[span, :])

    def table_by_x(kx):
        kh, kl = div(kx, XL), rem(kx, XL)
        span = pl.ds(pl.multiple_of(NQ * HALF + kl * (Y * HALF), HALF), Y * HALF)
        block = jnp.concatenate([flat(gath_a[1, ky, kl, kh]) for ky in range(Y)], axis=1).astype(BF16)
        pair[pl.ds(pl.multiple_of(S + kh * ZR, ZR), ZR), span] = block
        logits[columns(kh, ZR), :] += rows_dot(block, tok_t[span, :])

    big[1].wait()
    turn(og, og_t, 0)
    arrive(swaps[1])
    turn(og, og_t, 1)
    table_by_y(y)
    table_by_x(x)
    arrive(*last)
    for i in far_first:
        table_by_y(rem(y + N - i, N))
        table_by_x(rem(x + N - i, N))
    lg = logits[...]

    slots_b = jnp.max(lg, axis=0, keepdims=True)
    raised = jnp.exp(lg - slots_b)
    sums_b = jnp.sum(raised, axis=0, keepdims=True)
    wide = lax.broadcasted_iota(jnp.int32, (8, 2 * T), 0)
    line[0] = jnp.where(wide == 0, slots_b, sums_b)
    line_move = group(line_rec.at[0])
    send(line_move, line.at[0], line_rec.at[0], other)
    top = jnp.max(lg, axis=1, keepdims=True)
    local = jnp.exp(lg - top)
    total = jnp.sum(local, axis=1, keepdims=True)
    lanes = lax.broadcasted_iota(jnp.int32, (S, 128), 1)
    stat[0] = jnp.where(lanes == 0, top, jnp.where(lanes == 1, total, 0.0)).T[0:8]
    stats = [group(stat_p)]
    for n, step in enumerate(plane):
        send(stats[0], stat.at[0], stat_p.at[n], plane_to(*step))
    local_b = local.astype(BF16)

    def place(target, a, ky, kl, values):
        for hh in range(XH):
            block = values[hh * ZR : hh * ZR + ZR].reshape(Z, 8, values.shape[1]).astype(BF16)
            if a == 0:
                target[0, ky, hh * XL + kl] = block
            else:
                target[1, hh * XL + kl, ky] = block

    for ky in range(Y):
        values = rows_dot(local_b, tok[:, ky * XL * W : (ky + 1) * XL * W])
        for kl in range(XL):
            place(pb, 0, ky, kl, values[:, kl * W : (kl + 1) * W])
    moves = spread(pb, rb1, 0)

    arrive(line_move)
    got = line_rec[0]
    got = jnp.concatenate([got[:, T:], got[:, :T]], axis=1)
    high = jnp.maximum(slots_b, got[0:1])
    low = jnp.exp(slots_b - high)
    share = low / (sums_b * low + got[1:2] * jnp.exp(got[0:1] - high))
    comb = raised * share
    weight[...] = comb
    comb_b = comb.astype(BF16)
    for k in range(Y):
        values = rows_dot(comb_b, og[:, 2 * k * W : 2 * (k + 1) * W])
        for e in range(2):
            place(pb, 1, (2 * k + e) % Y, (2 * k + e) // Y, values[:, e * W : (e + 1) * W])
    moves.update(spread(pb, rb1, 1))
    sum_chunk, grad_chunk = end_of(reduce(pb, pb2, pb3, rb1, rb2, rbz, moves, stats))

    sum_chunk = sum_chunk / scale_in[pl.ds(own_row, 8), Z + 1 : Z + 2]
    seq_in[q, 0] = sum_chunk.astype(BF16)
    seq_in[q, 1] = grad_chunk.astype(BF16)
    before = len(groups) - 1
    seq_move = group(seq_in.at[0 : NQ - 1])
    for step in seq_far_first:
        send(seq_move, seq_in.at[q], seq_in.at[q], seq_to(*step)[1])
    sent(before)
    big[2].wait()
    big[3].wait()
    upper = lax.broadcasted_iota(jnp.int32, (8, 1), 0) < 4

    def pick(f, g):
        return jnp.where(upper, f, g)

    pre = hid_grad = None
    for step in ((0, 0),) + seq_far_first:
        if step == seq_far_first[0]:
            arrive(seq_move)
        k = seq_from(*step)
        slot_b, grad_b = (seq_in[k, a].astype(F32).astype(BF16) for a in range(2))
        more = [rows_dot(slot_b, win[e, columns(k, W), :]) for e in range(2)]
        pre = more if pre is None else [f + g for f, g in zip(pre, more)]
        more = [cols_dot(grad_b, wout[e, :, columns(by_x(k), W)]) for e in range(2)]
        hid_grad = more if hid_grad is None else [f + g for f, g in zip(hid_grad, more)]
    hidden, slope = gelu_and_slope(pick(*pre))
    hidden = hidden.astype(BF16)
    act = (pick(*hid_grad) * slope).astype(BF16)

    def products(step):
        k, device = seq_to(*step)
        in_part = pick(*(cols_dot(act, win[e, columns(k, W), :]) for e in range(2)))
        out_part = pick(*(rows_dot(hidden, wout[e, :, columns(by_x(k), W)]) for e in range(2)))
        return k, device, in_part.astype(BF16), out_part.astype(BF16)

    seq_move = group(seq_rec)
    order = seq_far_first + ((0, 0),)
    ready = products(order[0])
    for n, step in enumerate(order):
        k, device, in_part, out_part = ready
        if n + 1 < len(order):
            ready = products(order[n + 1])
        seq_out[k, 0] = in_part
        seq_out[k, 1] = out_part
        if step != (0, 0):
            send(seq_move, seq_out.at[k], seq_rec.at[step[0] * XL + step[1] - 1], device)
    arrive(seq_move)
    for a in (1, 0):
        total = seq_out[q, a].astype(F32)
        for i in range(NQ - 1):
            total += seq_rec[i, a].astype(F32)
        own_d[a] = total.astype(BF16)
    part = jnp.sum(sum_chunk * total.astype(BF16).astype(F32), axis=1, keepdims=True)
    spots = lax.broadcasted_iota(jnp.int32, (8, S), 1)
    cen[0] = jnp.where(spots == own_row + lines, part, 0.0)
    steps = gather(own_d, gath_d, (cen, cen_z, cen_p))
    next(steps)
    sent(seq_move + 1)
    *_, last = steps

    comb_g[...] = jnp.zeros_like(comb_g)
    disp_g[...] = jnp.zeros_like(disp_g)

    def back_disp(ky):
        span = columns(ky, XL * W)
        block = jnp.concatenate([flat(gath_d[0, ky, kl]) for kl in range(XL)], axis=1).astype(BF16)
        pair[0:S, span] = block
        disp_g[...] += rows_dot(block, tok_t[span, :])

    def back_comb(kx):
        kh, kl = div(kx, XL), rem(kx, XL)
        block = jnp.concatenate([flat(gath_d[1, ky, kl, kh]) for ky in range(Y)], axis=1).astype(BF16)
        comb_g[columns(kh, ZR), :] += rows_dot(block, og_t[columns(kl, Y * W), :])

    back_comb(x)
    back_disp(y)
    arrive(*last)
    for i in far_first:
        back_comb(rem(x + N - i, N))
    comb = weight[...]
    comb_grad = comb_g[...]
    mean = jnp.sum(comb * comb_grad, axis=0, keepdims=True)
    line[1] = jnp.broadcast_to(mean, (8, 2 * T))
    line_move = group(line_rec.at[1])
    send(line_move, line.at[1], line_rec.at[1], other)
    for i in far_first:
        back_disp(rem(y + N - i, N))
    centre_row = cen[1]
    for n in range(N * N - 1):
        centre_row += cen_p[n]
    centre = jnp.broadcast_to(jnp.sum(centre_row, axis=0, keepdims=True), (128, S)).T[:, 0:1]
    disp = jnp.exp(logits[...] - scale_out[:, Z : Z + 1]) / scale_out[:, Z + 1 : Z + 2]
    disp_part = disp * (disp_g[...] - centre)
    arrive(line_move)
    got = line_rec[1]
    mean = mean + jnp.concatenate([got[:, T:], got[:, :T]], axis=1)[0:1]
    logit_grad = disp_part + comb * (comb_grad - mean)
    logit_b = logit_grad.astype(BF16)

    for ky in range(Y):
        values = rows_dot(logit_b, tok[:, ky * XL * W : (ky + 1) * XL * W])
        for kl in range(XL):
            for a in range(2):
                place(pg, a, ky, kl, values[:, (2 * kl + a) * HALF : (2 * kl + a + 1) * HALF])
    moves = {**spread(pg, rg1, 0), **spread(pg, rg1, 1)}
    both[:, 0:S] = disp.T.astype(BF16)
    both[:, S : 2 * S] = logit_grad.T.astype(BF16)

    def their_grads(k, _):
        tg_send[:, columns(k, W)] = rows_dot(both[T : 2 * T], pair[:, columns(k, W)]).astype(BF16)
        return 0

    lax.fori_loop(0, NQ, their_grads, 0)
    tg_move = group(tg_rec)
    send(tg_move, tg_send, tg_rec, other)
    steps = reduce(pg, pg2, pg3, rg1, rg2, rgz, moves)
    next(steps)
    arrive(tg_move)

    def own_grads(k, _):
        span = columns(k, W)
        tg[:, span] = (rows_dot(both[0:T], pair[:, span]) + tg_rec[:, span].astype(F32)).astype(BF16)
        return 0

    lax.fori_loop(0, NQ, own_grads, 0)
    next(steps)
    sent(len(groups) - 1)
    parts = end_of(steps)
    for a in range(2):
        sg_out[:, a * HALF : (a + 1) * HALF] = parts[a]
    sent(len(groups))
    assert len(groups) == send_sem.shape[0], len(groups)


def shards(sizes, tokens, slot_embed, expert_in, expert_out, out_grad):
    Y, XL, Z, XH, C = sizes
    N, NQ = XL * XH, Y * XL
    T, D = tokens.shape
    S = slot_embed.shape[1] * Z * XH
    W = D // NQ
    H = W // 2
    vm = pltpu.VMEM

    def reduce_buffers(w):
        return [
            vm((2, N, N, Z, 8, w), BF16),
            vm((2, N, Z, 8, w), BF16),
            vm((2, Z, 8, w), BF16),
            vm((2, N - 1, N, Z, 8, w), BF16),
            vm((2, N - 1, Z, 8, w), BF16),
            vm((Z, 2, 8, w), BF16),
        ]

    n = 42
    scratch = [
        vm((2 * T, D), BF16), vm((2 * T, D), BF16), vm(expert_in.shape, BF16), vm(expert_out.shape, BF16),
        vm((D, 2 * T), BF16), vm((D, 2 * T), BF16), vm((2 * S, D), BF16),
        vm((S, 2 * T), F32), vm((S, 2 * T), F32), vm((S, 2 * T), F32), vm((S, 2 * T), F32),
        vm((2 * T, 2 * S), BF16), vm((T, D), BF16), vm((T, D), BF16),
        vm((2, 8, H), BF16), vm((2, 8, W), BF16), vm((2, Y, XL, XH, Z, 8, H), BF16), vm((2, Y, XL, XH, Z, 8, W), BF16),
        *reduce_buffers(W), *reduce_buffers(H),
        vm((2, 8, S), F32), vm((N * N - 1, 8, S), F32), vm((Z - 1, 8, S), F32),
        vm((2, S, 128), F32), vm((S, 128), F32), vm((S, 128), F32),
        vm((2, 8, S), F32), vm((Z, 8, S), F32), vm((N * N - 1, 8, S), F32),
        vm((NQ, 2, 8, W), BF16), vm((NQ, 2, 8, W), BF16), vm((NQ - 1, 2, 8, W), BF16),
        vm((2, 8, 2 * T), F32), vm((2, 8, 2 * T), F32),
        pltpu.SemaphoreType.DMA((6,)), pltpu.SemaphoreType.DMA((n,)), pltpu.SemaphoreType.DMA((n,)),
    ]
    hbm = pl.BlockSpec(memory_space=pl.ANY)
    tok_grad, slot_grad = pl.pallas_call(
        functools.partial(kernel, sizes),
        out_shape=(pltpu.VMEM((T, D), BF16), pltpu.VMEM((8, W), F32)),
        in_specs=[hbm] * 5,
        out_specs=(pl.BlockSpec(memory_space=pltpu.VMEM), pl.BlockSpec(memory_space=pltpu.VMEM)),
        scratch_shapes=scratch,
        compiler_params=pltpu.CompilerParams(collective_id=0, has_side_effects=True),
        name="soft_moe",
    )(tokens, slot_embed.T, expert_in, expert_out, out_grad)
    return tok_grad, slot_grad.T


SIZES = (4, 2, 8, 2, 2)


def solution(mesh, sizes=SIZES):
    torus = Mesh(mesh.devices.reshape(sizes), AXES)
    placed = (
        P(SEQ_EXP, None),
        P(None, EXP),
        P(EXP, None, SEQ),
        P(EXP, SEQ, None),
        P(SEQ_EXP, None),
    )
    return jax.shard_map(
        functools.partial(shards, sizes),
        mesh=torus,
        in_specs=placed,
        out_specs=(P(SEQ_EXP, None), P(SEQ, EXP)),
        check_vma=False,
    )
```

```python
import functools

import jax
import jax.numpy as jnp
from jax import lax
from jax.experimental import pallas as pl
from jax.experimental.pallas import tpu as pltpu
from jax.sharding import Mesh
from jax.sharding import PartitionSpec as P

EXP = ("exp_0", "exp_1", "exp_2")
SEQ = ("seq_0", "seq_1")
SEQ_EXP = ("seq_0", "seq_1", "exp_0", "exp_1", "exp_2")
AXES = SEQ_EXP
F32, BF16 = jnp.float32, jnp.bfloat16
ROOT = 0.7978845608028654


def rows_dot(left, right):
    return lax.dot_general(left, right, (((1,), (0,)), ((), ())), preferred_element_type=F32)


def cols_dot(left, right):
    return lax.dot_general(left, right, (((1,), (1,)), ((), ())), preferred_element_type=F32)


def gelu_and_slope(v):
    t = jnp.tanh(ROOT * (v + 0.044715 * (v * v * v)))
    value = 0.5 * v * (1.0 + t)
    slope = 0.5 * (1.0 + t) + 0.5 * v * (1.0 - t * t) * (ROOT * (1.0 + 3.0 * 0.044715 * (v * v)))
    return value, slope


def flat(block):
    block = block.astype(F32)
    return block.reshape(-1, block.shape[-1])


def kernel(
    sizes,
    tok_hbm, slot_hbm, win_hbm, wout_hbm, og_hbm,
    tg, sg_out,
    tok, og, win, wout, tok_t, og_t, pair, logits, weight, comb_g, disp_g, both, tg_send, tg_rec,
    own_a, own_s, own_g, gath_a, gath_s, gath_g,
    ps, ps2, ps3, rs1, rs2, rsz,
    pw, pw2, pw3, rw1, rw2, rwz,
    pg, pg2, pg3, rg1, rg2, rgz,
    stat, stat_p, stat_z, factor, scale_out, scale_in,
    cen, cen_z, cen_p,
    in_s, in_g, out_s, out_g, rec_s, rec_g, line, line_rec,
    local_sem, send_sem, recv_sem,
):
    Y, XL, Z, XH, C = sizes
    N, NQ = XL * XH, Y * XL
    assert Y == N and C == 2 and XL == 2 and XH == 2
    S = XH * Z * 8
    T = tok.shape[0] // 2
    W = tok.shape[1] // NQ
    HALF = W // 2
    ZR = Z * 8
    y, xl, z, xh, c = (lax.axis_index(name) for name in AXES)
    x, q = xh * XL + xl, y * XL + xl
    rem, div = lax.rem, lax.div

    def z_to(i):
        k = rem(z + i, Z)
        return k, {"exp_0": k}

    def owner_to(i):
        k = rem(z + i, Z)
        return k, {"exp_0": k, "exp_2": 1 - c}

    def y_to(i):
        k = rem(y + i, N)
        return k, {"seq_0": k}

    def x_to(i):
        k = rem(x + i, N)
        return k, {"exp_1": div(k, XL), "seq_1": rem(k, XL)}

    def plane_to(dy, dx):
        kx = rem(x + dx, N)
        return {"seq_0": rem(y + dy, N), "exp_1": div(kx, XL), "seq_1": rem(kx, XL)}

    def seq_to(dy, dl):
        ky, kl = rem(y + dy, N), rem(xl + dl, XL)
        return ky * XL + kl, {"seq_0": ky, "seq_1": kl}

    def seq_from(dy, dl):
        return rem(y + N - dy, N) * XL + rem(xl + dl, XL)

    other = {"exp_2": 1 - c}
    far_first = (2, 1, 3)
    z_far_first = sorted(range(Z), key=lambda i: -min(i, Z - i))
    plane = [(dy, dx) for dy in (2, 1, 3, 0) for dx in (2, 1, 3, 0) if dy or dx]
    seq_far_first = ((2, 1), (2, 0), (1, 1), (3, 1), (1, 0), (3, 0), (0, 1))
    MESH = pl.DeviceIdType.MESH
    groups, over = [], [0]

    def group(whole):
        groups.append(whole)
        return len(groups) - 1

    def send(k, src, dst, device):
        pltpu.make_async_remote_copy(
            src_ref=src, dst_ref=dst, send_sem=send_sem.at[k], recv_sem=recv_sem.at[k],
            device_id=device, device_id_type=MESH,
        ).start()

    def arrive(*which):
        for k in which:
            pltpu.make_async_copy(groups[k], groups[k], recv_sem.at[k]).wait()

    def sent(n):
        for k in range(over[0], n):
            pltpu.make_async_copy(groups[k], groups[k], send_sem.at[k]).wait()
        over[0] = max(n, over[0])

    def columns(k, width):
        return pl.ds(pl.multiple_of(k * width, width), width)

    mine, theirs = pl.ds(0, T), pl.ds(T, T)
    first = [
        pltpu.make_async_copy(
            slot_hbm.at[:, columns(start, HALF)],
            own_a.at[a],
            local_sem.at[a],
        )
        for a, start in ((0, xl * Y + y), (1, NQ + y * XL + xl))
    ]
    big = [
        pltpu.make_async_copy(src, dst, local_sem.at[2 + k])
        for k, (src, dst) in enumerate(
            ((tok_hbm, tok.at[mine]), (og_hbm, og.at[mine]), (win_hbm, win), (wout_hbm, wout))
        )
    ]
    for copy in first + big:
        copy.start()

    barrier = pltpu.get_barrier_semaphore()
    partners = [z_to(i)[1] for i in range(1, Z)] + [owner_to(i)[1] for i in range(1, Z)]
    partners += [plane_to(*step) for step in plane]
    partners += [other]
    for device in partners:
        pl.semaphore_signal(barrier, inc=1, device_id=device, device_id_type=MESH)
    for copy in first:
        copy.wait()
    pl.semaphore_wait(barrier, len(partners))

    def gather(block, buf, beside=None):
        along = [group(buf.at[:, y, xl, xh])]
        for i in z_far_first:
            send(along[0], block, buf.at[:, y, xl, xh, z], owner_to(i)[1])
        if beside:
            own, over_z, over_plane = beside
            along.append(group(over_z))
            for i in z_far_first:
                send(along[1], own.at[0], over_z.at[i], owner_to(i)[1])
        yield
        arrive(*along)
        hops = {}
        for i in far_first:
            hops[i] = group(buf.at[:, y, xl, xh])
            send(hops[i], buf.at[0, y, xl, xh], buf.at[0, y, xl, xh], x_to(i)[1])
            send(hops[i], buf.at[1, y, xl, xh], buf.at[1, y, xl, xh], y_to(i)[1])
        last = {}

        def pass_on(j):
            last[j] = group(buf.at[:, 0 : N - 1, 0, 0])
            kx = rem(x + N - j, N)
            part = buf.at[0, y, rem(kx, XL), div(kx, XL)]
            for i in far_first:
                send(last[j], part, part, y_to(i)[1])
            part = buf.at[1, rem(y + N - j, N), xl, xh]
            for i in far_first:
                send(last[j], part, part, x_to(i)[1])

        pass_on(0)
        if beside:
            total = over_z[0]
            for i in range(1, Z):
                total += over_z[i]
            own[1] = total
            last["rows"] = group(over_plane)
            for n, step in enumerate(plane):
                send(last["rows"], own.at[1], over_plane.at[n], plane_to(*step))
        yield
        for j in (1, 3, 2):
            arrive(hops[j])
            pass_on(j)
        yield last

    lines = lax.broadcasted_iota(jnp.int32, (8, S), 0)

    def merge(entries):
        top = entries[0][0]
        for entry in entries[1:]:
            top = jnp.maximum(top, entry[0])
        scales = [jnp.exp(entry[0] - top) for entry in entries]
        total = entries[0][1] * scales[0]
        for entry, scale in zip(entries[1:], scales[1:]):
            total += entry[1] * scale
        return (top, total), scales

    def upright(rows):
        turned = jnp.zeros((16, S), F32)
        tall = lax.broadcasted_iota(jnp.int32, (16, S), 0)
        for k, row in enumerate(rows):
            turned = jnp.where(tall == k, row, turned)
        return jnp.concatenate([turned, jnp.zeros((112, S), F32)], axis=0).T

    def joined(parts, scale, row, rows):
        total = None
        for k, part in enumerate(parts):
            part = flat(part)
            if scale is not None:
                part = part * scale[pl.ds(pl.multiple_of(row, 8), rows), k : k + 1]
            total = part if total is None else total + part
        return total

    def reduce(p, s2, s3, r1, r2, rz, moves, stats=None):
        w = p.shape[-1]
        scaled = stats is not None
        if scaled:
            arrive(*stats)
            halves = lambda e: (e[:, 0:S], e[:, S : 2 * S])
            stat_of = {(0, 0): stat[0]}
            for n, step in enumerate(plane):
                stat_of[step] = stat_p[n]
            by_y = [merge([halves(stat_of[i, j]) for i in range(N)]) for j in range(N)]
            by_x = [merge([halves(stat_of[i, j]) for j in range(N)]) for i in range(N)]
            merged, across_x = merge([joint for joint, _ in by_y])
            _, across_y = merge([joint for joint, _ in by_x])
            stat[1] = jnp.concatenate(merged, axis=1)
            stats = [group(stat_z)]
            for i in z_far_first:
                if i:
                    send(stats[0], stat.at[1], stat_z.at[i - 1], z_to(i)[1])
            for k, rows in enumerate((by_y[0][1], by_x[0][1], across_x, across_y)):
                factor[k] = upright(rows)
        later = [group(r2)]
        for j in far_first + (0,):
            for a, me, (b, device) in ((0, y, x_to(j)), (1, x, y_to(j))):
                arrive(moves[a, j])
                parts = [p[a, me, b]] + [r1[a, i, b] for i in range(N - 1)]
                row = (div(b, XL) if a == 0 else xh) * ZR
                total = joined(parts, factor.at[a] if scaled else None, row, ZR)
                s2[a, b] = total.reshape(Z, 8, w).astype(BF16)
                if j:
                    send(later[0], s2.at[a, b], r2.at[a, j - 1], device)
        moves = later
        yield
        if scaled:
            arrive(*stats)
            entries = [stat[1]] + [stat_z[i] for i in range(Z - 1)]
            merged, across = merge([halves(e) for e in entries])
            scale_out[...] = upright(across + list(merged))
            scale_move = group(scale_in)
            send(scale_move, scale_out, scale_in, other)
        arrive(*moves)
        for a, me in ((0, x), (1, y)):
            parts = [s2[a, me]] + [r2[a, i] for i in range(N - 1)]
            total = joined(parts, factor.at[2 + a] if scaled else None, xh * ZR, ZR)
            s3[a] = total.reshape(Z, 8, w).astype(BF16)
        moves = [group(rz)]
        for i in z_far_first:
            k, device = owner_to(i)
            send(moves[0], s3.at[:, k], rz.at[i], device)
        if scaled:
            moves.append(scale_move)
        yield
        arrive(*moves)
        result = []
        for a in range(2):
            parts = [rz[i, a] for i in range(Z)]
            result.append(joined(parts, scale_in if scaled else None, own_row, 8))
        yield result

    def spread(p, r1, a):
        first_to, then_to = (y_to, x_to) if a == 0 else (x_to, y_to)
        moves = {}
        for j in far_first + (0,):
            b = then_to(j)[0]
            moves[a, j] = group(r1.at[a, :, b])
            for i in far_first:
                k, device = first_to(i)
                send(moves[a, j], p.at[a, k, b], r1.at[a, i - 1, b], device)
        return moves

    def end_of(steps):
        last = None
        for last in steps:
            pass
        return last

    own_row = pl.multiple_of(xh * ZR + z * 8, 8)

    def turn(source, target, half):
        target[:, half * T : half * T + T] = source[half * T : half * T + T].T

    steps = gather(own_a, gath_a)
    next(steps)
    swaps = [group(tok.at[theirs]), group(og.at[theirs])]
    send(swaps[0], tok_hbm, tok.at[theirs], other)
    big[0].wait()
    turn(tok, tok_t, 0)
    next(steps)
    send(swaps[1], og_hbm, og.at[theirs], other)
    arrive(swaps[0])
    turn(tok, tok_t, 1)
    last = next(steps)
    logits[...] = jnp.zeros_like(logits)

    def use_table(j):
        ky, kx = rem(y + N - j, N), rem(x + N - j, N)
        kh, kl = div(kx, XL), rem(kx, XL)
        span = columns(kl, Y * HALF)
        block = jnp.concatenate([flat(gath_a[0, k, kl, kh]) for k in range(Y)], axis=1).astype(BF16)
        pair[pl.ds(pl.multiple_of(S + kh * ZR, ZR), ZR), span] = block
        logits[columns(kh, ZR), :] += rows_dot(block, tok_t[span, :])
        span = pl.ds(pl.multiple_of(NQ * HALF + ky * (XL * HALF), HALF), XL * HALF)
        block = jnp.concatenate([flat(gath_a[1, ky, k]) for k in range(XL)], axis=1).astype(BF16)
        pair[S : 2 * S, span] = block
        logits[...] += rows_dot(block, tok_t[span, :])

    big[1].wait()
    turn(og, og_t, 0)
    arrive(swaps[1])
    turn(og, og_t, 1)
    for j in (0, 1, 3, 2):
        arrive(last[j])
        use_table(j)
    lg = logits[...]

    slots_b = jnp.max(lg, axis=0, keepdims=True)
    raised = jnp.exp(lg - slots_b)
    sums_b = jnp.sum(raised, axis=0, keepdims=True)
    wide = lax.broadcasted_iota(jnp.int32, (8, 2 * T), 0)
    line[0] = jnp.where(wide == 0, slots_b, sums_b)
    line_move = group(line_rec.at[0])
    send(line_move, line.at[0], line_rec.at[0], other)
    top = jnp.max(lg, axis=1, keepdims=True)
    local = jnp.exp(lg - top)
    total = jnp.sum(local, axis=1, keepdims=True)
    lanes = lax.broadcasted_iota(jnp.int32, (S, 128), 1)
    turned = jnp.where(lanes == 0, top, jnp.where(lanes == 1, total, 0.0)).T
    stat[0] = jnp.concatenate([turned[0:1], turned[1:2]], axis=1)
    stats = [group(stat_p)]
    for n, step in enumerate(plane):
        send(stats[0], stat.at[0], stat_p.at[n], plane_to(*step))
    local_b = local.astype(BF16)

    def place(target, a, ky, kl, values):
        for hh in range(XH):
            block = values[hh * ZR : hh * ZR + ZR].reshape(Z, 8, values.shape[1]).astype(BF16)
            if a == 0:
                target[0, ky, hh * XL + kl] = block
            else:
                target[1, hh * XL + kl, ky] = block

    def partial_sums(rows, patches, p, r1):
        for ky in range(Y):
            values = rows_dot(rows, patches[:, ky * XL * W : (ky + 1) * XL * W])
            for kl in range(XL):
                for a in range(2):
                    place(p, a, ky, kl, values[:, (2 * kl + a) * HALF : (2 * kl + a + 1) * HALF])
        return {**spread(p, r1, 0), **spread(p, r1, 1)}

    slot_moves = partial_sums(local_b, tok, ps, rs1)

    arrive(line_move)
    got = line_rec[0]
    got = jnp.concatenate([got[:, T:], got[:, :T]], axis=1)
    high = jnp.maximum(slots_b, got[0:1])
    low = jnp.exp(slots_b - high)
    share = low / (sums_b * low + got[1:2] * jnp.exp(got[0:1] - high))
    comb = raised * share
    weight[...] = comb
    comb_b = comb.astype(BF16)
    grad_moves = partial_sums(comb_b, og, pw, rw1)

    slot_steps = reduce(ps, ps2, ps3, rs1, rs2, rsz, slot_moves, stats)
    grad_steps = reduce(pw, pw2, pw3, rw1, rw2, rwz, grad_moves)
    next(slot_steps)
    next(grad_steps)
    next(slot_steps)
    next(grad_steps)
    before = len(groups) - 2
    upper = lax.broadcasted_iota(jnp.int32, (8, 1), 0) < 4
    seq_rings = (((2, 1),), ((2, 0), (1, 1), (3, 1)), ((1, 0), (3, 0), (0, 1)))
    order = seq_far_first + ((0, 0),)

    def pick(f, g):
        return jnp.where(upper, f, g)

    def seq_send(buf):
        moves = {}
        for ring in seq_rings:
            moves[ring[0]] = group(buf.at[0 : len(ring)])
            for step in ring:
                send(moves[ring[0]], buf.at[q], buf.at[q], seq_to(*step)[1])
        return moves

    def seq_use(buf, moves, product):
        total = None
        for step in ((0, 0),) + sum(seq_rings[::-1], ()):
            if step in moves:
                arrive(moves[step])
            k = seq_from(*step)
            rows = buf[k].astype(F32).astype(BF16)
            more = [product(rows, e, columns(k, W)) for e in range(2)]
            total = more if total is None else [f + g for f, g in zip(total, more)]
        return pick(*total)

    def seq_give(buf, rec, product):
        move = group(rec)
        ready = product(columns(seq_to(*order[0])[0], W))
        for n, step in enumerate(order):
            now = ready
            if n + 1 < len(order):
                ready = product(columns(seq_to(*order[n + 1])[0], W))
            k, device = seq_to(*step)
            buf[k] = now.astype(BF16)
            if step != (0, 0):
                send(move, buf.at[k], rec.at[step[0] * XL + step[1] - 1], device)
        return move

    def seq_sum(buf, rec, target):
        total = buf[q].astype(F32)
        for i in range(NQ - 1):
            total += rec[i].astype(F32)
        total = total.astype(BF16)
        for a in range(2):
            target[a] = total[:, a * HALF : (a + 1) * HALF]
        return total.astype(F32)

    sum_chunk = jnp.concatenate(next(slot_steps), axis=1) / scale_in[pl.ds(own_row, 8), Z + 1 : Z + 2]
    in_s[q] = sum_chunk.astype(BF16)
    slot_moves = seq_send(in_s)
    in_g[q] = jnp.concatenate(next(grad_steps), axis=1).astype(BF16)
    grad_moves = seq_send(in_g)
    sent(before)
    big[2].wait()
    big[3].wait()
    pre = seq_use(in_s, slot_moves, lambda rows, e, span: rows_dot(rows, win[e, span, :]))
    hidden, slope = gelu_and_slope(pre)
    hidden = hidden.astype(BF16)
    slot_move = seq_give(out_s, rec_s, lambda span: pick(*(rows_dot(hidden, wout[e, :, span]) for e in range(2))))
    hid_grad = seq_use(in_g, grad_moves, lambda rows, e, span: cols_dot(rows, wout[e, :, span]))
    act = (hid_grad * slope).astype(BF16)
    grad_move = seq_give(out_g, rec_g, lambda span: pick(*(cols_dot(act, win[e, span, :]) for e in range(2))))
    arrive(slot_move)
    seq_sum(out_s, rec_s, own_s)
    slot_steps = gather(own_s, gath_s)
    next(slot_steps)
    arrive(grad_move)
    total = seq_sum(out_g, rec_g, own_g)
    part = jnp.sum(sum_chunk * total, axis=1, keepdims=True)
    spots = lax.broadcasted_iota(jnp.int32, (8, S), 1)
    cen[0] = jnp.sum(jnp.where(spots == own_row + lines, part, 0.0), axis=0, keepdims=True)
    grad_steps = gather(own_g, gath_g, (cen, cen_z, cen_p))
    next(grad_steps)
    sent(grad_move + 1)
    next(slot_steps)
    next(grad_steps)
    slot_last = next(slot_steps)
    grad_last = next(grad_steps)

    comb_g[...] = jnp.zeros_like(comb_g)
    disp_g[...] = jnp.zeros_like(disp_g)

    def back(j, buf, right, target, keep):
        ky, kx = rem(y + N - j, N), rem(x + N - j, N)
        kh, kl = div(kx, XL), rem(kx, XL)
        for a, rows, spots in (
            (0, columns(kh, ZR), [(k, kl) for k in range(Y)]),
            (1, pl.ds(0, S), [(ky, k) for k in range(XL)]),
        ):
            spans = [pl.ds(pl.multiple_of((f * XL + g) * W + a * HALF, HALF), HALF) for f, g in spots]
            blocks = [flat(buf[0, f, g, kh] if a == 0 else buf[1, f, g]) for f, g in spots]
            if keep:
                for span, block in zip(spans, blocks):
                    pair[rows, span] = block.astype(BF16)
            block = jnp.concatenate(blocks, axis=1).astype(BF16)
            target[rows, :] += rows_dot(block, jnp.concatenate([right[span, :] for span in spans], axis=0))

    for j in (0, 1, 3, 2):
        arrive(slot_last[j])
        back(j, gath_s, og_t, comb_g, False)
    comb = weight[...]
    comb_grad = comb_g[...]
    mean = jnp.sum(comb * comb_grad, axis=0, keepdims=True)
    line[1] = jnp.broadcast_to(mean, (8, 2 * T))
    line_move = group(line_rec.at[1])
    send(line_move, line.at[1], line_rec.at[1], other)
    for j in (0, 1, 3, 2):
        arrive(grad_last[j])
        back(j, gath_g, tok_t, disp_g, True)
    arrive(grad_last["rows"])
    centre_row = cen[1]
    for n in range(N * N - 1):
        centre_row += cen_p[n]
    centre = jnp.broadcast_to(centre_row, (128, S)).T[:, 0:1]
    disp = jnp.exp(logits[...] - scale_out[:, Z : Z + 1]) / scale_out[:, Z + 1 : Z + 2]
    disp_part = disp * (disp_g[...] - centre)
    arrive(line_move)
    got = line_rec[1]
    mean = mean + jnp.concatenate([got[:, T:], got[:, :T]], axis=1)[0:1]
    logit_grad = disp_part + comb * (comb_grad - mean)
    logit_b = logit_grad.astype(BF16)

    moves = partial_sums(logit_b, tok, pg, rg1)
    both[:, 0:S] = disp.T.astype(BF16)
    both[:, S : 2 * S] = logit_grad.T.astype(BF16)

    def their_grads(k, _):
        tg_send[:, columns(k, W)] = rows_dot(both[T : 2 * T], pair[:, columns(k, W)]).astype(BF16)
        return 0

    lax.fori_loop(0, NQ, their_grads, 0)
    tg_move = group(tg_rec)
    send(tg_move, tg_send, tg_rec, other)
    steps = reduce(pg, pg2, pg3, rg1, rg2, rgz, moves)
    next(steps)
    arrive(tg_move)

    def own_grads(k, _):
        span = columns(k, W)
        tg[:, span] = (rows_dot(both[0:T], pair[:, span]) + tg_rec[:, span].astype(F32)).astype(BF16)
        return 0

    lax.fori_loop(0, NQ, own_grads, 0)
    next(steps)
    sent(len(groups) - 1)
    parts = end_of(steps)
    for a in range(2):
        sg_out[:, a * HALF : (a + 1) * HALF] = parts[a]
    sent(len(groups))
    assert len(groups) == send_sem.shape[0], len(groups)


def shards(sizes, tokens, slot_embed, expert_in, expert_out, out_grad):
    Y, XL, Z, XH, C = sizes
    N, NQ = XL * XH, Y * XL
    T, D = tokens.shape
    S = slot_embed.shape[1] * Z * XH
    W = D // NQ
    H = W // 2
    vm = pltpu.VMEM

    def reduce_buffers(w):
        return [
            vm((2, N, N, Z, 8, w), BF16),
            vm((2, N, Z, 8, w), BF16),
            vm((2, Z, 8, w), BF16),
            vm((2, N - 1, N, Z, 8, w), BF16),
            vm((2, N - 1, Z, 8, w), BF16),
            vm((Z, 2, 8, w), BF16),
        ]

    n = 72
    scratch = [
        vm((2 * T, D), BF16), vm((2 * T, D), BF16), vm(expert_in.shape, BF16), vm(expert_out.shape, BF16),
        vm((D, 2 * T), BF16), vm((D, 2 * T), BF16), vm((2 * S, D), BF16),
        vm((S, 2 * T), F32), vm((S, 2 * T), F32), vm((S, 2 * T), F32), vm((S, 2 * T), F32),
        vm((2 * T, 2 * S), BF16), vm((T, D), BF16), vm((T, D), BF16),
        *[vm((2, 8, H), BF16)] * 3, *[vm((2, Y, XL, XH, Z, 8, H), BF16)] * 3,
        *reduce_buffers(H), *reduce_buffers(H), *reduce_buffers(H),
        vm((2, 1, 2 * S), F32), vm((N * N - 1, 1, 2 * S), F32), vm((Z - 1, 1, 2 * S), F32),
        vm((4, S, 128), F32), vm((S, 128), F32), vm((S, 128), F32),
        vm((2, 1, S), F32), vm((Z, 1, S), F32), vm((N * N - 1, 1, S), F32),
        *[vm((NQ, 8, W), BF16)] * 4, *[vm((NQ - 1, 8, W), BF16)] * 2,
        vm((2, 8, 2 * T), F32), vm((2, 8, 2 * T), F32),
        pltpu.SemaphoreType.DMA((6,)), pltpu.SemaphoreType.DMA((n,)), pltpu.SemaphoreType.DMA((n,)),
    ]
    hbm = pl.BlockSpec(memory_space=pl.ANY)
    tok_grad, slot_grad = pl.pallas_call(
        functools.partial(kernel, sizes),
        out_shape=(pltpu.VMEM((T, D), BF16), pltpu.VMEM((8, W), F32)),
        in_specs=[hbm] * 5,
        out_specs=(pl.BlockSpec(memory_space=pltpu.VMEM), pl.BlockSpec(memory_space=pltpu.VMEM)),
        scratch_shapes=scratch,
        compiler_params=pltpu.CompilerParams(collective_id=0, has_side_effects=True),
        name="soft_moe",
    )(tokens, slot_embed.T, expert_in, expert_out, out_grad)
    return tok_grad, slot_grad.T


SIZES = (4, 2, 8, 2, 2)


def solution(mesh, sizes=SIZES):
    torus = Mesh(mesh.devices.reshape(sizes), AXES)
    placed = (
        P(SEQ_EXP, None),
        P(None, EXP),
        P(EXP, None, SEQ),
        P(EXP, SEQ, None),
        P(SEQ_EXP, None),
    )
    return jax.shard_map(
        functools.partial(shards, sizes),
        mesh=torus,
        in_specs=placed,
        out_specs=(P(SEQ_EXP, None), P(SEQ, EXP)),
        check_vma=False,
    )
```
